32 devices in a mesh: dp: 2 (over x), tp: 4 (over z), sp: 4 (over y, core).
Axes of the slice: x: 2, y: 2, z: 4, core: 2. Of those that a mesh axis runs over, the one named last changes fastest.
Arguments:
- hidden: bfloat16 [512, 4096], P('dp'), parts along dimension 0
- lengths: int32 [512], P('dp'), parts along dimension 0
- k_cache: bfloat16 [512, 128, 8, 128], P('dp', 'sp', 'tp'), parts along dimension 0
- v_cache: bfloat16 [512, 128, 8, 128], P('dp', 'sp', 'tp'), parts along dimension 0
- norm_gain: bfloat16 [4096], replicated
- w_query: bfloat16 [4096, 4096], P(None, 'tp')
- w_key: bfloat16 [4096, 1024], P(None, 'tp')
- w_value: bfloat16 [4096, 1024], P(None, 'tp')
- w_out: bfloat16 [4096, 4096], P('tp')
Outputs:
- output 1: bfloat16 [512, 4096], P('dp'), parts along dimension 0
- output 2: bfloat16 [512, 128, 8, 128], P('dp', 'sp', 'tp'), parts along dimension 0
- output 3: bfloat16 [512, 128, 8, 128], P('dp', 'sp', 'tp'), parts along dimension 0
There are 2 independent parts. The reference program is written for one: setup_inputs(seed, part) draws one part's arguments, and reference() takes and returns one part's arrays. A program takes and returns all parts, laid end to end along the dimension named above; an argument that names none is the same for every part.
All inputs are finite; a program needn't handle non-finite values.
Results may differ from the reference program's by a relative error of at most 0.00451752.
Values sent between devices are 32-bit elements.
A program may use at most 1 GiB of HBM per device.

```python
import jax
import jax.numpy as jnp
from jax import lax

D_MODEL = 4096
HEADS = 32
KV_HEADS = 8
HEAD_DIM = 128
BATCH = 256
SEQ_LEN = 128

GROUP_SIZE = HEADS // KV_HEADS
SCALE = HEAD_DIM ** -0.5
EPS = 1e-6
NEG_BIG = -1e30


def setup_inputs(seed: int = 0, part: int = 0) -> dict:
    part_keys = jax.random.split(jax.random.fold_in(jax.random.key(seed), part), 4)
    shared_keys = jax.random.split(jax.random.key(seed + 1), 5)
    cache_shape = (BATCH, SEQ_LEN, KV_HEADS, HEAD_DIM)
    hidden = jax.random.normal(part_keys[0], (BATCH, D_MODEL), jnp.float32)
    lengths = jax.random.randint(part_keys[1], (BATCH,), 0, SEQ_LEN, jnp.int32)
    lengths = lengths.at[0].set(SEQ_LEN - 1)
    k_cache = jax.random.normal(part_keys[2], cache_shape, jnp.float32)
    steps = jax.random.normal(part_keys[3], cache_shape, jnp.float32)
    v_cache = jnp.cumsum(steps, axis=1) * (2.0 / SEQ_LEN) ** 0.5 + steps
    norm_gain = 1.0 + 0.5 * jax.random.normal(shared_keys[0], (D_MODEL,), jnp.float32)
    w_query = jax.random.normal(shared_keys[1], (D_MODEL, HEADS * HEAD_DIM), jnp.float32) * D_MODEL ** -0.5
    w_key = jax.random.normal(shared_keys[2], (D_MODEL, KV_HEADS * HEAD_DIM), jnp.float32) * D_MODEL ** -0.5
    w_value = jax.random.normal(shared_keys[3], (D_MODEL, KV_HEADS * HEAD_DIM), jnp.float32) * D_MODEL ** -0.5
    w_out = jax.random.normal(shared_keys[4], (HEADS * HEAD_DIM, D_MODEL), jnp.float32) * (HEADS * HEAD_DIM) ** -0.5
    return {
        'hidden': hidden.astype(jnp.bfloat16),
        'lengths': lengths,
        'k_cache': k_cache.astype(jnp.bfloat16),
        'v_cache': v_cache.astype(jnp.bfloat16),
        'norm_gain': norm_gain.astype(jnp.bfloat16),
        'w_query': w_query.astype(jnp.bfloat16),
        'w_key': w_key.astype(jnp.bfloat16),
        'w_value': w_value.astype(jnp.bfloat16),
        'w_out': w_out.astype(jnp.bfloat16),
    }


def reference(hidden, lengths, k_cache, v_cache, norm_gain, w_query, w_key, w_value, w_out):
    hid_f32 = hidden.astype(jnp.float32)
    inv_rms = lax.rsqrt(jnp.mean(hid_f32 * hid_f32, axis=-1, keepdims=True) + EPS)
    normed = (hid_f32 * inv_rms * norm_gain.astype(jnp.float32)).astype(jnp.bfloat16)
    query = jnp.dot(normed, w_query, preferred_element_type=jnp.float32).astype(jnp.bfloat16)
    new_key = jnp.dot(normed, w_key, preferred_element_type=jnp.float32).astype(jnp.bfloat16)
    new_value = jnp.dot(normed, w_value, preferred_element_type=jnp.float32).astype(jnp.bfloat16)
    positions = jnp.arange(SEQ_LEN)
    at_slot = (positions[None, :] == lengths[:, None])[:, :, None, None]
    k_new = jnp.where(at_slot, new_key.reshape(BATCH, 1, KV_HEADS, HEAD_DIM), k_cache)
    v_new = jnp.where(at_slot, new_value.reshape(BATCH, 1, KV_HEADS, HEAD_DIM), v_cache)
    query_groups = query.reshape(BATCH, KV_HEADS, GROUP_SIZE, HEAD_DIM)

    def one_sequence(item):
        q_seq, k_seq, v_seq, length = item
        scores = jnp.einsum('kgd,tkd->kgt', q_seq.astype(jnp.float32), k_seq.astype(jnp.float32)) * SCALE
        valid = positions <= length
        scores = jnp.where(valid, scores, NEG_BIG)
        peak = jnp.max(scores, axis=-1, keepdims=True)
        exp_vals = jnp.where(valid, jnp.exp(scores - peak), 0.0)
        denom_sum = jnp.sum(exp_vals, axis=-1, keepdims=True)
        weighted = jnp.einsum('kgt,tkd->kgd', exp_vals.astype(jnp.bfloat16).astype(jnp.float32), v_seq.astype(jnp.float32))
        return (weighted / denom_sum).astype(jnp.bfloat16)

    attn_out = lax.map(one_sequence, (query_groups, k_new, v_new, lengths))
    proj_sum = jnp.dot(attn_out.reshape(BATCH, HEADS * HEAD_DIM), w_out, preferred_element_type=jnp.float32)
    hidden_out = (hid_f32 + proj_sum).astype(jnp.bfloat16)
    return (hidden_out, k_new, v_new)
```

```python
import functools

import jax
import jax.numpy as jnp
from jax import lax
from jax.experimental import pallas as pl
from jax.experimental.pallas import tpu as pltpu
from jax.sharding import PartitionSpec as P

EPS = 1e-6
NEG_BIG = -1e30
MESH = pl.DeviceIdType.MESH
HALVES = 2
COLS = 512


def combine_kernel(acc_ref, stats_ref, hid_ref, w_hbm, out_ref, w_ref, stat_in, fac_ref, d2d_in, y_out, y_in, obuf, pbuf,
                   pe_in, abuf, mb_in, fall, w_sem, st_s, st_r, dd_s, dd_r, yy_s, yy_r, p_s, p_r, a_s, a_r, fz_s, fz_r,
                   fy_s, fy_r, fs_s, fs_r, gs_s, gs_r):
    heads = acc_ref.shape[1] // 128
    rows = obuf.shape[1]
    own_rows = HALVES * rows
    per_half = out_ref.shape[1] // COLS
    chunks = HALVES * per_half
    sp = lax.axis_index('sp')
    z = lax.axis_index('tp')
    y, c = sp // 2, sp % 2
    sib, yn, diag = 2 * y + (1 - c), 2 * (1 - y) + c, 2 * (1 - y) + (1 - c)
    inner = jnp.logical_or(z == 1, z == 2)
    is_end = jnp.logical_or(z == 0, z == 3)
    low = z // 2
    end_z = low * 3
    mid_z = 2 - low
    inner_z = 1 + low

    pltpu.make_async_copy(w_hbm, w_ref, w_sem).start()

    barrier = pltpu.get_barrier_semaphore()
    for peer in (sib, yn, diag):
        pl.semaphore_signal(barrier, inc=1, device_id={'sp': peer}, device_id_type=MESH)

    @pl.when(inner)
    def _():
        pl.semaphore_signal(barrier, inc=1, device_id={'tp': end_z}, device_id_type=MESH)
        pl.semaphore_signal(barrier, inc=1, device_id={'tp': mid_z}, device_id_type=MESH)
        pl.semaphore_wait(barrier, 5)

    @pl.when(is_end)
    def _():
        pl.semaphore_signal(barrier, inc=1, device_id={'tp': inner_z}, device_id_type=MESH)
        pl.semaphore_wait(barrier, 4)

    def remote(src, dst, send, recv, **where):
        return pltpu.make_async_remote_copy(src_ref=src, dst_ref=dst, send_sem=send, recv_sem=recv, device_id=where,
                                            device_id_type=MESH)

    def stat_copy(i, peer):
        lanes = pl.ds(pl.multiple_of((peer % 2) * 2 * own_rows, 128), 2 * own_rows)
        return remote(stats_ref.at[:, lanes], stat_in.at[i], st_s.at[i], st_r.at[i], sp=peer)

    stat_copies = [stat_copy(i, peer) for i, peer in enumerate((sib, yn, diag))]
    for copy in stat_copies:
        copy.start()

    def d2d_copy(t, r):
        plane = (1 - y) if t == 0 else y
        start = pl.multiple_of((1 - c) * 2 * own_rows + plane * own_rows + r * rows, rows)
        return remote(acc_ref.at[pl.ds(start, rows), :], d2d_in.at[t, r], dd_s.at[2 * r + t], dd_r.at[2 * r + t], sp=sib)

    d2d_copies = [[d2d_copy(t, r) for r in range(HALVES)] for t in range(2)]
    for r in range(HALVES):
        for t in range(2):
            d2d_copies[t][r].start()

    for copy in stat_copies:
        copy.wait()
    lanes = pl.ds(pl.multiple_of(c * 2 * own_rows, 128), 2 * own_rows)
    peaks = [stats_ref[0:heads, lanes]] + [stat_in[i, 0:heads, :] for i in range(3)]
    sums = [stats_ref[heads:2 * heads, lanes]] + [stat_in[i, heads:2 * heads, :] for i in range(3)]
    top = jnp.maximum(jnp.maximum(peaks[0], peaks[1]), jnp.maximum(peaks[2], peaks[3]))
    weights = [jnp.exp(peak - top) for peak in peaks]
    total = sums[0] * weights[0] + sums[1] * weights[1] + (sums[2] * weights[2] + sums[3] * weights[3])
    factors = jnp.concatenate(
        [weights[0] / total, weights[1] / total, jnp.zeros((2 * own_rows - 2 * heads, 2 * own_rows), jnp.float32)], axis=0)
    fac_ref[...] = factors.T

    def combined(t, r, j):
        plane = (1 - y) if t == 0 else y
        base = pl.multiple_of(plane * own_rows + r * rows, rows)
        start = pl.multiple_of(c * 2 * own_rows + base, rows)
        cols = slice(j * 128, (j + 1) * 128)
        mine = acc_ref[pl.ds(start, rows), cols] * fac_ref[pl.ds(base, rows), j:j + 1]
        return mine + d2d_in[t, r, :, cols] * fac_ref[pl.ds(base, rows), heads + j:heads + j + 1]

    def y_copy(r):
        return remote(y_out.at[r], y_in.at[r], yy_s.at[r], yy_r.at[r], sp=yn)

    y_copies = [y_copy(r) for r in range(HALVES)]
    for r in range(HALVES):
        d2d_copies[0][r].wait()
        for j in range(heads):
            y_out[r, :, j * 128:(j + 1) * 128] = combined(0, r, j)
        y_copies[r].start()

    def p_copy(k):
        return remote(pbuf.at[k], pe_in.at[k], p_s.at[k], p_r.at[k], tp=inner_z)

    def a_copy(k):
        return remote(abuf.at[k], mb_in.at[k], a_s.at[k], a_r.at[k], tp=mid_z)

    def fz_copy(k):
        return remote(fall.at[sp, k], fall.at[sp, k], fz_s.at[k], fz_r.at[k], tp=end_z)

    def fy_copy(k, owner):
        return remote(fall.at[owner, k], fall.at[owner, k], fy_s.at[k], fy_r.at[k], sp=yn)

    def fs_copy(k, owner):
        return remote(fall.at[owner, k], fall.at[owner, k], fs_s.at[k], fs_r.at[k], sp=sib)

    def gs_copy(k, owner):
        return remote(fall.at[owner, k], fall.at[owner, k], gs_s.at[k], gs_r.at[k], sp=sib)

    for r in range(HALVES):
        d2d_copies[1][r].wait()
        y_copies[r].wait()
        for j in range(heads):
            obuf[r, :, j * 128:(j + 1) * 128] = (combined(1, r, j) + y_in[r, :, j * 128:(j + 1) * 128]).astype(jnp.bfloat16)
        if r == 0:
            pltpu.make_async_copy(w_hbm, w_ref, w_sem).wait()
        for j in range(per_half):
            k = r * per_half + j
            pbuf[k] = jnp.dot(obuf[r], w_ref[:, j * COLS:(j + 1) * COLS], preferred_element_type=jnp.float32)

            @pl.when(is_end)
            def _():
                p_copy(k).start()

    def stage_a(k):
        @pl.when(inner)
        def _():
            p_copy(k).wait_recv()
            abuf[k] = pbuf[k] + pe_in[k]
            a_copy(k).start()

    def stage_f(k):
        @pl.when(inner)
        def _():
            a_copy(k).wait_recv()
            fall[sp, k] = abuf[k] + mb_in[k]
            fz_copy(k).start()

        @pl.when(is_end)
        def _():
            fz_copy(k).wait_recv()

        fy_copy(k, sp).start()
        fs_copy(k, sp).start()

    def stage_y(k):
        fy_copy(k, yn).wait_recv()
        gs_copy(k, yn).start()

    def stage_o(k):
        fs_copy(k, sib).wait_recv()
        gs_copy(k, diag).wait_recv()
        r, j = k // per_half, k % per_half
        cols = slice(j * COLS, (j + 1) * COLS)
        for owner in range(4):
            oy, oc = owner // 2, owner % 2
            start = oc * 2 * own_rows + oy * own_rows + r * rows
            out_ref[start:start + rows, cols] = (
                hid_ref[start:start + rows, cols].astype(jnp.float32) + fall[owner, k]).astype(jnp.bfloat16)

    stages = ((stage_a, 0), (stage_f, 2), (stage_y, 4), (stage_o, 6))
    for step in range(chunks + 6):
        for stage, lag in stages:
            if 0 <= step - lag < chunks:
                stage(step - lag)

    for k in range(chunks):
        @pl.when(inner)
        def _():
            a_copy(k).wait_send()
            fz_copy(k).wait_send()

        @pl.when(is_end)
        def _():
            p_copy(k).wait_send()

        fy_copy(k, sp).wait_send()
        fs_copy(k, sp).wait_send()
        gs_copy(k, yn).wait_send()


def combine(acc, stats, hidden, w_out):
    batch, width = acc.shape
    features = w_out.shape[1]
    rows = batch // (4 * HALVES)
    chunks = HALVES * (features // COLS)
    dma = lambda *shape: pltpu.SemaphoreType.DMA(shape)
    f32 = lambda *shape: pltpu.VMEM(shape, jnp.float32)
    vmem = pl.BlockSpec(memory_space=pltpu.VMEM)
    return pl.pallas_call(
        combine_kernel,
        out_shape=jax.ShapeDtypeStruct((batch, features), jnp.bfloat16),
        in_specs=[vmem, vmem, vmem, pl.BlockSpec(memory_space=pl.ANY)],
        out_specs=vmem,
        scratch_shapes=[
            pltpu.VMEM(w_out.shape, jnp.bfloat16),
            f32(3, stats.shape[0], batch // 2),
            f32(batch // 2, batch // 2),
            f32(2, HALVES, rows, width),
            f32(HALVES, rows, width),
            f32(HALVES, rows, width),
            pltpu.VMEM((HALVES, rows, width), jnp.bfloat16),
            f32(chunks, rows, COLS),
            f32(chunks, rows, COLS),
            f32(chunks, rows, COLS),
            f32(chunks, rows, COLS),
            f32(4, chunks, rows, COLS),
            pltpu.SemaphoreType.DMA,
            dma(3), dma(3), dma(2 * HALVES), dma(2 * HALVES), dma(HALVES), dma(HALVES),
        ] + [dma(chunks)] * 12,
        compiler_params=pltpu.CompilerParams(collective_id=0, has_side_effects=True, vmem_limit_bytes=60 * 2**20),
        name='combine',
    )(acc, stats, hidden, w_out)


def solution(mesh):
    cache_spec = P('dp', 'sp', 'tp', None)

    def local_step(hidden, lengths, k_cache, v_cache, norm_gain, w_query, w_key, w_value, w_out):
        batch, seq_block, kv_local, head_dim = k_cache.shape
        heads_local = w_query.shape[1] // head_dim
        group = heads_local // kv_local
        hid_f32 = hidden.astype(jnp.float32)
        inv_rms = lax.rsqrt(jnp.mean(hid_f32 * hid_f32, axis=-1, keepdims=True) + EPS)
        normed = (hid_f32 * inv_rms * norm_gain.astype(jnp.float32)).astype(jnp.bfloat16)
        query = jnp.dot(normed, w_query, preferred_element_type=jnp.float32).astype(jnp.bfloat16)
        query = query.reshape(batch, kv_local, group, head_dim)
        new_key = jnp.dot(normed, w_key, preferred_element_type=jnp.float32).astype(jnp.bfloat16)
        new_value = jnp.dot(normed, w_value, preferred_element_type=jnp.float32).astype(jnp.bfloat16)
        positions = lax.axis_index('sp') * seq_block + jnp.arange(seq_block)
        at_slot = (positions[None, :] == lengths[:, None])[:, :, None, None]
        k_new = jnp.where(at_slot, new_key.reshape(batch, 1, kv_local, head_dim), k_cache)
        v_new = jnp.where(at_slot, new_value.reshape(batch, 1, kv_local, head_dim), v_cache)
        scores = jnp.einsum('bkgd,btkd->bkgt', query, k_new, preferred_element_type=jnp.float32) * (head_dim ** -0.5)
        valid = (positions[None, :] <= lengths[:, None])[:, None, None, :]
        scores = jnp.where(valid, scores, NEG_BIG)
        local_peak = jnp.max(scores, axis=-1, keepdims=True)
        exp_vals = jnp.where(valid, jnp.exp(scores - local_peak), 0.0)
        local_denom = jnp.sum(exp_vals, axis=-1, keepdims=True)
        local_acc = jnp.einsum('bkgt,btkd->bkgd', exp_vals.astype(jnp.bfloat16), v_new, preferred_element_type=jnp.float32)
        stats = jnp.concatenate([local_peak.reshape(batch, heads_local), local_denom.reshape(batch, heads_local)], axis=1).T
        hidden_out = combine(local_acc.reshape(batch, heads_local * head_dim), stats, hidden, w_out)
        return hidden_out, k_new, v_new

    return jax.shard_map(
        local_step,
        mesh=mesh,
        in_specs=(P('dp', None), P('dp'), cache_spec, cache_spec, P(None), P(None, 'tp'), P(None, 'tp'), P(None, 'tp'), P('tp', None)),
        out_specs=(P('dp', None), cache_spec, cache_spec),
        check_vma=False,
    )
```

```python
import jax
import jax.numpy as jnp
from jax import lax
from jax.experimental import pallas as pl
from jax.experimental.pallas import tpu as pltpu
from jax.sharding import PartitionSpec as P

EPS = 1e-6
NEG_BIG = -1e30
MESH = pl.DeviceIdType.MESH
HALVES = 2
COLS = 512
BLOCK = 32
SCALE = 128 ** -0.5


def combine_kernel(acc_ref, stats_ref, hid_ref, w_hbm, out_ref, w_ref, stat_in, fac_ref, d2d_in, y_out, y_in, obuf, pbuf,
                   pe_in, abuf, mb_in, fall, w_sem, st_s, st_r, dd_s, dd_r, yy_s, yy_r, p_s, p_r, a_s, a_r, fz_s, fz_r,
                   fy_s, fy_r, fs_s, fs_r, gs_s, gs_r):
    heads = acc_ref.shape[1] // 128
    rows = obuf.shape[1]
    own_rows = HALVES * rows
    per_half = out_ref.shape[1] // COLS
    chunks = HALVES * per_half
    sp = lax.axis_index('sp')
    z = lax.axis_index('tp')
    y, c = sp // 2, sp % 2
    sib, yn, diag = 2 * y + (1 - c), 2 * (1 - y) + c, 2 * (1 - y) + (1 - c)
    inner = jnp.logical_or(z == 1, z == 2)
    is_end = jnp.logical_or(z == 0, z == 3)
    low = z // 2
    end_z = low * 3
    mid_z = 2 - low
    inner_z = 1 + low

    pltpu.make_async_copy(w_hbm, w_ref, w_sem).start()

    barrier = pltpu.get_barrier_semaphore()
    for peer in (sib, yn, diag):
        pl.semaphore_signal(barrier, inc=1, device_id={'sp': peer}, device_id_type=MESH)

    @pl.when(inner)
    def _():
        pl.semaphore_signal(barrier, inc=1, device_id={'tp': end_z}, device_id_type=MESH)
        pl.semaphore_signal(barrier, inc=1, device_id={'tp': mid_z}, device_id_type=MESH)
        pl.semaphore_wait(barrier, 5)

    @pl.when(is_end)
    def _():
        pl.semaphore_signal(barrier, inc=1, device_id={'tp': inner_z}, device_id_type=MESH)
        pl.semaphore_wait(barrier, 4)

    def remote(src, dst, send, recv, **where):
        return pltpu.make_async_remote_copy(src_ref=src, dst_ref=dst, send_sem=send, recv_sem=recv, device_id=where,
                                            device_id_type=MESH)

    def stat_copy(i, peer):
        lanes = pl.ds(pl.multiple_of((peer % 2) * 2 * own_rows, 128), 2 * own_rows)
        return remote(stats_ref.at[:, lanes], stat_in.at[i], st_s.at[i], st_r.at[i], sp=peer)

    stat_copies = [stat_copy(i, peer) for i, peer in enumerate((sib, yn, diag))]
    for copy in stat_copies:
        copy.start()

    def d2d_copy(t, r):
        plane = (1 - y) if t == 0 else y
        start = pl.multiple_of((1 - c) * 2 * own_rows + plane * own_rows + r * rows, rows)
        return remote(acc_ref.at[pl.ds(start, rows), :], d2d_in.at[t, r], dd_s.at[2 * r + t], dd_r.at[2 * r + t], sp=sib)

    d2d_copies = [[d2d_copy(t, r) for r in range(HALVES)] for t in range(2)]
    for r in range(HALVES):
        for t in range(2):
            d2d_copies[t][r].start()

    for copy in stat_copies:
        copy.wait()
    lanes = pl.ds(pl.multiple_of(c * 2 * own_rows, 128), 2 * own_rows)
    peaks = [stats_ref[0:heads, lanes]] + [stat_in[i, 0:heads, :] for i in range(3)]
    sums = [stats_ref[heads:2 * heads, lanes]] + [stat_in[i, heads:2 * heads, :] for i in range(3)]
    top = jnp.maximum(jnp.maximum(peaks[0], peaks[1]), jnp.maximum(peaks[2], peaks[3]))
    weights = [jnp.exp(peak - top) for peak in peaks]
    total = sums[0] * weights[0] + sums[1] * weights[1] + (sums[2] * weights[2] + sums[3] * weights[3])
    factors = jnp.concatenate(
        [weights[0] / total, weights[1] / total, jnp.zeros((2 * own_rows - 2 * heads, 2 * own_rows), jnp.float32)], axis=0)
    fac_ref[...] = factors.T

    def combined(t, r, j):
        plane = (1 - y) if t == 0 else y
        base = pl.multiple_of(plane * own_rows + r * rows, rows)
        start = pl.multiple_of(c * 2 * own_rows + base, rows)
        cols = slice(j * 128, (j + 1) * 128)
        mine = acc_ref[pl.ds(start, rows), cols] * fac_ref[pl.ds(base, rows), j:j + 1]
        return mine + d2d_in[t, r, :, cols] * fac_ref[pl.ds(base, rows), heads + j:heads + j + 1]

    def y_copy(r):
        return remote(y_out.at[r], y_in.at[r], yy_s.at[r], yy_r.at[r], sp=yn)

    y_copies = [y_copy(r) for r in range(HALVES)]
    for r in range(HALVES):
        d2d_copies[0][r].wait()
        for j in range(heads):
            y_out[r, :, j * 128:(j + 1) * 128] = combined(0, r, j)
        y_copies[r].start()

    def p_copy(k):
        return remote(pbuf.at[k], pe_in.at[k], p_s.at[k], p_r.at[k], tp=inner_z)

    def a_copy(k):
        return remote(abuf.at[k], mb_in.at[k], a_s.at[k], a_r.at[k], tp=mid_z)

    def fz_copy(k):
        return remote(fall.at[sp, k], fall.at[sp, k], fz_s.at[k], fz_r.at[k], tp=end_z)

    def fy_copy(k, owner):
        return remote(fall.at[owner, k], fall.at[owner, k], fy_s.at[k], fy_r.at[k], sp=yn)

    def fs_copy(k, owner):
        return remote(fall.at[owner, k], fall.at[owner, k], fs_s.at[k], fs_r.at[k], sp=sib)

    def gs_copy(k, owner):
        return remote(fall.at[owner, k], fall.at[owner, k], gs_s.at[k], gs_r.at[k], sp=sib)

    for r in range(HALVES):
        d2d_copies[1][r].wait()
        y_copies[r].wait()
        for j in range(heads):
            obuf[r, :, j * 128:(j + 1) * 128] = (combined(1, r, j) + y_in[r, :, j * 128:(j + 1) * 128]).astype(jnp.bfloat16)
        if r == 0:
            pltpu.make_async_copy(w_hbm, w_ref, w_sem).wait()
        for j in range(per_half):
            k = r * per_half + j
            pbuf[k] = jnp.dot(obuf[r], w_ref[:, j * COLS:(j + 1) * COLS], preferred_element_type=jnp.float32)

            @pl.when(is_end)
            def _():
                p_copy(k).start()

    def stage_a(k):
        @pl.when(inner)
        def _():
            p_copy(k).wait_recv()
            abuf[k] = pbuf[k] + pe_in[k]
            a_copy(k).start()

    def stage_f(k):
        @pl.when(inner)
        def _():
            a_copy(k).wait_recv()
            fall[sp, k] = abuf[k] + mb_in[k]
            fz_copy(k).start()

        @pl.when(is_end)
        def _():
            fz_copy(k).wait_recv()

        fy_copy(k, sp).start()
        fs_copy(k, sp).start()

    def stage_y(k):
        fy_copy(k, yn).wait_recv()
        gs_copy(k, yn).start()

    def stage_o(k):
        fs_copy(k, sib).wait_recv()
        gs_copy(k, diag).wait_recv()
        r, j = k // per_half, k % per_half
        cols = slice(j * COLS, (j + 1) * COLS)
        for owner in range(4):
            oy, oc = owner // 2, owner % 2
            start = oc * 2 * own_rows + oy * own_rows + r * rows
            out_ref[start:start + rows, cols] = (
                hid_ref[start:start + rows, cols].astype(jnp.float32) + fall[owner, k]).astype(jnp.bfloat16)

    stages = ((stage_a, 0), (stage_f, 2), (stage_y, 4), (stage_o, 6))
    for step in range(chunks + 6):
        for stage, lag in stages:
            if 0 <= step - lag < chunks:
                stage(step - lag)

    for k in range(chunks):
        @pl.when(inner)
        def _():
            a_copy(k).wait_send()
            fz_copy(k).wait_send()

        @pl.when(is_end)
        def _():
            p_copy(k).wait_send()

        fy_copy(k, sp).wait_send()
        fs_copy(k, sp).wait_send()
        gs_copy(k, yn).wait_send()


def combine(acc, stats, hidden, w_out):
    batch, width = acc.shape
    features = w_out.shape[1]
    rows = batch // (4 * HALVES)
    chunks = HALVES * (features // COLS)
    dma = lambda *shape: pltpu.SemaphoreType.DMA(shape)
    f32 = lambda *shape: pltpu.VMEM(shape, jnp.float32)
    vmem = pl.BlockSpec(memory_space=pltpu.VMEM)
    return pl.pallas_call(
        combine_kernel,
        out_shape=jax.ShapeDtypeStruct((batch, features), jnp.bfloat16),
        in_specs=[vmem, vmem, vmem, pl.BlockSpec(memory_space=pl.ANY)],
        out_specs=vmem,
        scratch_shapes=[
            pltpu.VMEM(w_out.shape, jnp.bfloat16),
            f32(3, stats.shape[0], batch // 2),
            f32(batch // 2, batch // 2),
            f32(2, HALVES, rows, width),
            f32(HALVES, rows, width),
            f32(HALVES, rows, width),
            pltpu.VMEM((HALVES, rows, width), jnp.bfloat16),
            f32(chunks, rows, COLS),
            f32(chunks, rows, COLS),
            f32(chunks, rows, COLS),
            f32(chunks, rows, COLS),
            f32(4, chunks, rows, COLS),
            pltpu.SemaphoreType.DMA,
            dma(3), dma(3), dma(2 * HALVES), dma(2 * HALVES), dma(HALVES), dma(HALVES),
        ] + [dma(chunks)] * 12,
        compiler_params=pltpu.CompilerParams(collective_id=0, has_side_effects=True, vmem_limit_bytes=60 * 2**20),
        name='combine',
    )(acc, stats, hidden, w_out)


def attend_kernel(len_smem, len_ref, hid_hbm, gain_ref, wq_hbm, wk_hbm, wv_hbm, k_hbm, v_hbm, kout_hbm, vout_hbm, acc_ref,
                  stats_ref, hid, nbuf, wq, wk, wv, kbuf, vbuf, qbuf, pair_f32, nk, nv, statbuf, hid_sem, wq_sem, wk_sem, wv_sem,
                  k_sem, v_sem, ko_sem, vo_sem):
    batch, features = hid.shape
    heads = qbuf.shape[1] // 128
    slots = batch * BLOCK
    base = lax.axis_index('sp') * BLOCK
    pieces = k_sem.shape[0]
    piece = slots // pieces
    copy = pltpu.make_async_copy
    quarter = batch // hid_sem.shape[0]
    hid_copies = [copy(hid_hbm.at[pl.ds(i * quarter, quarter), :], hid.at[pl.ds(i * quarter, quarter), :], hid_sem.at[i])
                  for i in range(hid_sem.shape[0])]
    wk_copy, wv_copy = copy(wk_hbm, wk, wk_sem), copy(wv_hbm, wv, wv_sem)
    wide = wq.shape[2]
    wq_copies = [copy(wq_hbm.at[:, pl.ds(i * wide, wide)], wq.at[i], wq_sem.at[i]) for i in range(wq.shape[0])]
    for c in hid_copies + [wk_copy, wv_copy] + wq_copies:
        c.start()

    def block_copy(src, dst, sem, i, step=piece):
        rows = pl.ds(pl.multiple_of(i * step, step), step)
        return copy(src.at[rows], dst.at[rows], sem.at[i])

    for i in range(pieces):
        block_copy(k_hbm, kbuf, k_sem, i).start()
        block_copy(v_hbm, vbuf, v_sem, i).start()

    gain = gain_ref[...].astype(jnp.float32)

    def norm_rows(i):
        rows = pl.ds(pl.multiple_of(i * 16, 16), 16)
        h = hid[rows, :].astype(jnp.float32)
        inv_rms = lax.rsqrt(jnp.mean(h * h, axis=-1, keepdims=True) + EPS)
        nbuf[rows, :] = (h * inv_rms * gain).astype(jnp.bfloat16)

    for i, c in enumerate(hid_copies):
        c.wait()
        per = quarter // 16
        pl.loop(i * per, (i + 1) * per)(norm_rows)

    for weight, weight_copy, out in ((wk, wk_copy, nk), (wv, wv_copy, nv)):
        weight_copy.wait()
        new = jnp.dot(nbuf[...], weight[...], preferred_element_type=jnp.float32)
        for j in range(2):
            pair_f32[pl.ds(j, batch, stride=2), :] = new[:, j * 128:(j + 1) * 128]
        out.reshape(2 * batch, 128)[...] = pair_f32[...].astype(jnp.bfloat16)

    for i, c in enumerate(wq_copies):
        c.wait()
        query = jnp.dot(nbuf[...], wq[i], preferred_element_type=jnp.float32)
        qbuf[:, i * wide:(i + 1) * wide] = query.astype(jnp.bfloat16).astype(jnp.float32)

    k_rows, v_rows = kbuf.reshape(kbuf.shape[0] * 2, 128), vbuf.reshape(vbuf.shape[0] * 2, 128)
    lane = lax.broadcasted_iota(jnp.int32, (8, 128), 1)
    row = lax.broadcasted_iota(jnp.int32, (8, 128), 0)
    slot_pos = base + (lane % 64) // 2
    own_seq = (lane // 64) == (row % 2)
    even = lane % 2 == 0
    pairs = [row // 2 == j for j in range(4)]

    def attend_tile(i):
        seqs = pl.ds(pl.multiple_of(i * 8, 8), 8)
        keys = pl.ds(pl.multiple_of(i * 512, 512), 512)
        q = jnp.concatenate([qbuf[seqs, h * 128:(h + 1) * 128] for h in range(heads)], axis=0).astype(jnp.bfloat16)
        s = lax.dot_general(q, k_rows[keys, :], (((1,), (1,)), ((), ())), preferred_element_type=jnp.float32)
        valid = jnp.logical_and(own_seq, slot_pos <= len_ref[seqs, :])
        valids = (jnp.logical_and(valid, even), jnp.logical_and(valid, jnp.logical_not(even)))
        stat = jnp.zeros((8, 128), jnp.float32)
        probs = []
        for h in range(heads):
            part = [s[h * 8:(h + 1) * 8, j * 128:(j + 1) * 128] for j in range(4)]
            score = jnp.where(pairs[0], part[0], jnp.where(pairs[1], part[1], jnp.where(pairs[2], part[2], part[3])))
            ok = valids[h // (heads // 2)]
            score = jnp.where(ok, score * SCALE, NEG_BIG)
            peak = jnp.max(score, axis=1, keepdims=True)
            e = jnp.where(ok, jnp.exp(score - peak), 0.0)
            stat = jnp.where(lane == h, peak, stat)
            stat = jnp.where(lane == heads + h, jnp.sum(e, axis=1, keepdims=True), stat)
            probs.append(jnp.concatenate([jnp.where(pairs[j], e, 0.0) for j in range(4)], axis=1))
        p = jnp.concatenate(probs, axis=0).astype(jnp.bfloat16)
        o = jnp.dot(p, v_rows[keys, :], preferred_element_type=jnp.float32)
        for h in range(heads):
            acc_ref[seqs, h * 128:(h + 1) * 128] = o[h * 8:(h + 1) * 8, :]
        statbuf[seqs, :] = stat

    @pl.loop(0, pieces)
    def _(i):
        block_copy(k_hbm, kbuf, k_sem, i).wait()
        block_copy(v_hbm, vbuf, v_sem, i).wait()
        seqs = piece // BLOCK

        @pl.loop(0, seqs, unroll=8)
        def _(j):
            b = i * seqs + j
            at = len_smem[b] - base
            slot = jnp.where(jnp.logical_and(at >= 0, at < BLOCK), b * BLOCK + at, slots)
            kbuf[slot] = nk[b]
            vbuf[slot] = nv[b]

        @pl.loop(0, seqs // 8, unroll=2)
        def _(j):
            attend_tile(i * (seqs // 8) + j)

        block_copy(kbuf, kout_hbm, ko_sem, i).start()
        block_copy(vbuf, vout_hbm, vo_sem, i).start()

    for i in range(batch // 128):
        stats_ref[:, i * 128:(i + 1) * 128] = statbuf[i * 128:(i + 1) * 128, :].T[0:2 * heads, :]

    for i in range(pieces):
        block_copy(kbuf, kout_hbm, ko_sem, i).wait()
        block_copy(vbuf, vout_hbm, vo_sem, i).wait()


def attend(hidden, lengths, k_cache, v_cache, norm_gain, w_query, w_key, w_value):
    batch, block, kv, dim = k_cache.shape
    features, width = w_query.shape
    slots = batch * block
    bf16 = lambda *shape: pltpu.VMEM(shape, jnp.bfloat16)
    f32 = lambda *shape: pltpu.VMEM(shape, jnp.float32)
    dma = lambda *shape: pltpu.SemaphoreType.DMA(shape)
    vmem, hbm = pl.BlockSpec(memory_space=pltpu.VMEM), pl.BlockSpec(memory_space=pl.ANY)
    cache = jax.ShapeDtypeStruct((slots, kv, dim), jnp.bfloat16)
    k_new, v_new, acc, stats = pl.pallas_call(
        attend_kernel,
        out_shape=[cache, cache, jax.ShapeDtypeStruct((batch, width), jnp.float32),
                   jax.ShapeDtypeStruct((2 * width // dim, batch), jnp.float32)],
        in_specs=[pl.BlockSpec(memory_space=pltpu.SMEM), vmem, hbm, vmem, hbm, hbm, hbm, hbm, hbm],
        out_specs=[hbm, hbm, vmem, vmem],
        scratch_shapes=[
            bf16(batch, features), bf16(batch, features), bf16(width // 256, features, 256), bf16(features, 256),
            bf16(features, 256), bf16(slots + 8, kv, dim), bf16(slots + 8, kv, dim), f32(batch, width), f32(2 * batch, dim),
            bf16(batch, kv, dim), bf16(batch, kv, dim), f32(batch, 128),
            dma(4), dma(width // 256), pltpu.SemaphoreType.DMA, pltpu.SemaphoreType.DMA, dma(8), dma(8), dma(8), dma(8),
        ],
        compiler_params=pltpu.CompilerParams(vmem_limit_bytes=60 * 2**20),
        name='attend',
    )(lengths, jnp.broadcast_to(lengths[:, None], (batch, 128)), hidden, norm_gain.reshape(1, features), w_query, w_key, w_value,
      k_cache.reshape(slots, kv, dim), v_cache.reshape(slots, kv, dim))
    return k_new.reshape(k_cache.shape), v_new.reshape(v_cache.shape), acc, stats


def solution(mesh):
    cache_spec = P('dp', 'sp', 'tp', None)

    def local_step(hidden, lengths, k_cache, v_cache, norm_gain, w_query, w_key, w_value, w_out):
        k_new, v_new, acc, stats = attend(hidden, lengths, k_cache, v_cache, norm_gain, w_query, w_key, w_value)
        return combine(acc, stats, hidden, w_out), k_new, v_new

    return jax.shard_map(
        local_step,
        mesh=mesh,
        in_specs=(P('dp', None), P('dp'), cache_spec, cache_spec, P(None), P(None, 'tp'), P(None, 'tp'), P(None, 'tp'), P('tp', None)),
        out_specs=(P('dp', None), cache_spec, cache_spec),
        check_vma=False,
    )
```

```python
import jax
import jax.numpy as jnp
from jax import lax
from jax.experimental import pallas as pl
from jax.experimental.pallas import tpu as pltpu
from jax.sharding import PartitionSpec as P

EPS = 1e-6
NEG_BIG = -1e30
MESH = pl.DeviceIdType.MESH
HALVES = 2
COLS = 512
BLOCK = 32
SCALE = 128 ** -0.5
UNROLL = 2
ATTEND_VMEM = 62.5
COMBINE_VMEM = 60.5


def combine_kernel(acc_ref, stats_ref, hid_hbm, w_hbm, out_ref, hid_ref, w_ref, stat_in, fac_ref, d2d_in, y_out, y_in, obuf, pbuf,
                   pe_in, abuf, mb_in, fall, h_sem, w_sem, st_s, st_r, dd_s, dd_r, yy_s, yy_r, p_s, p_r, a_s, a_r, fz_s, fz_r,
                   fy_s, fy_r, fs_s, fs_r, gs_s, gs_r):
    heads = acc_ref.shape[1] // 128
    rows = obuf.shape[1]
    own_rows = HALVES * rows
    per_half = out_ref.shape[1] // COLS
    chunks = HALVES * per_half
    sp = lax.axis_index('sp')
    z = lax.axis_index('tp')
    y, c = sp // 2, sp % 2
    sib, yn, diag = 2 * y + (1 - c), 2 * (1 - y) + c, 2 * (1 - y) + (1 - c)
    inner = jnp.logical_or(z == 1, z == 2)
    is_end = jnp.logical_or(z == 0, z == 3)
    low = z // 2
    end_z = low * 3
    mid_z = 2 - low
    inner_z = 1 + low

    hid_copy, w_copy = pltpu.make_async_copy(hid_hbm, hid_ref, h_sem), pltpu.make_async_copy(w_hbm, w_ref, w_sem)
    w_copy.start()
    hid_copy.start()

    barrier = pltpu.get_barrier_semaphore()
    for peer in (sib, yn, diag):
        pl.semaphore_signal(barrier, inc=1, device_id={'sp': peer}, device_id_type=MESH)

    @pl.when(inner)
    def _():
        pl.semaphore_signal(barrier, inc=1, device_id={'tp': end_z}, device_id_type=MESH)
        pl.semaphore_signal(barrier, inc=1, device_id={'tp': mid_z}, device_id_type=MESH)
        pl.semaphore_wait(barrier, 5)

    @pl.when(is_end)
    def _():
        pl.semaphore_signal(barrier, inc=1, device_id={'tp': inner_z}, device_id_type=MESH)
        pl.semaphore_wait(barrier, 4)

    def remote(src, dst, send, recv, **where):
        return pltpu.make_async_remote_copy(src_ref=src, dst_ref=dst, send_sem=send, recv_sem=recv, device_id=where,
                                            device_id_type=MESH)

    def stat_copy(i, peer):
        lanes = pl.ds(pl.multiple_of((peer % 2) * 2 * own_rows, 128), 2 * own_rows)
        return remote(stats_ref.at[:, lanes], stat_in.at[i], st_s.at[i], st_r.at[i], sp=peer)

    stat_copies = [stat_copy(i, peer) for i, peer in enumerate((sib, yn, diag))]
    for copy in stat_copies:
        copy.start()

    def d2d_copy(t, r):
        plane = (1 - y) if t == 0 else y
        start = pl.multiple_of((1 - c) * 2 * own_rows + plane * own_rows + r * rows, rows)
        return remote(acc_ref.at[pl.ds(start, rows), :], d2d_in.at[t, r], dd_s.at[2 * r + t], dd_r.at[2 * r + t], sp=sib)

    d2d_copies = [[d2d_copy(t, r) for r in range(HALVES)] for t in range(2)]
    for r in range(HALVES):
        for t in range(2):
            d2d_copies[t][r].start()

    for copy in stat_copies:
        copy.wait()
    lanes = pl.ds(pl.multiple_of(c * 2 * own_rows, 128), 2 * own_rows)
    peaks = [stats_ref[0:heads, lanes]] + [stat_in[i, 0:heads, :] for i in range(3)]
    sums = [stats_ref[heads:2 * heads, lanes]] + [stat_in[i, heads:2 * heads, :] for i in range(3)]
    top = jnp.maximum(jnp.maximum(peaks[0], peaks[1]), jnp.maximum(peaks[2], peaks[3]))
    weights = [jnp.exp(peak - top) for peak in peaks]
    total = sums[0] * weights[0] + sums[1] * weights[1] + (sums[2] * weights[2] + sums[3] * weights[3])
    factors = jnp.concatenate(
        [weights[0] / total, weights[1] / total, jnp.zeros((2 * own_rows - 2 * heads, 2 * own_rows), jnp.float32)], axis=0)
    fac_ref[...] = factors.T

    def combined(t, r, j):
        plane = (1 - y) if t == 0 else y
        base = pl.multiple_of(plane * own_rows + r * rows, rows)
        start = pl.multiple_of(c * 2 * own_rows + base, rows)
        cols = slice(j * 128, (j + 1) * 128)
        mine = acc_ref[pl.ds(start, rows), cols] * fac_ref[pl.ds(base, rows), j:j + 1]
        return mine + d2d_in[t, r, :, cols] * fac_ref[pl.ds(base, rows), heads + j:heads + j + 1]

    def y_copy(r):
        return remote(y_out.at[r], y_in.at[r], yy_s.at[r], yy_r.at[r], sp=yn)

    y_copies = [y_copy(r) for r in range(HALVES)]
    for r in range(HALVES):
        d2d_copies[0][r].wait()
        for j in range(heads):
            y_out[r, :, j * 128:(j + 1) * 128] = combined(0, r, j)
        y_copies[r].start()

    def p_copy(k):
        return remote(pbuf.at[k], pe_in.at[k], p_s.at[k], p_r.at[k], tp=inner_z)

    def a_copy(k):
        return remote(abuf.at[k], mb_in.at[k], a_s.at[k], a_r.at[k], tp=mid_z)

    def fz_copy(k):
        return remote(fall.at[sp, k], fall.at[sp, k], fz_s.at[k], fz_r.at[k], tp=end_z)

    def fy_copy(k, owner):
        return remote(fall.at[owner, k], fall.at[owner, k], fy_s.at[k], fy_r.at[k], sp=yn)

    def fs_copy(k, owner):
        return remote(fall.at[owner, k], fall.at[owner, k], fs_s.at[k], fs_r.at[k], sp=sib)

    def gs_copy(k, owner):
        return remote(fall.at[owner, k], fall.at[owner, k], gs_s.at[k], gs_r.at[k], sp=sib)

    for r in range(HALVES):
        if r == 0:
            w_copy.wait()
            hid_copy.wait()
        d2d_copies[1][r].wait()
        y_copies[r].wait()
        for j in range(heads):
            obuf[r, :, j * 128:(j + 1) * 128] = (combined(1, r, j) + y_in[r, :, j * 128:(j + 1) * 128]).astype(jnp.bfloat16)
        for j in range(per_half):
            k = r * per_half + j
            pbuf[k] = jnp.dot(obuf[r], w_ref[:, j * COLS:(j + 1) * COLS], preferred_element_type=jnp.float32)

            @pl.when(is_end)
            def _():
                p_copy(k).start()

    def stage_a(k):
        @pl.when(inner)
        def _():
            p_copy(k).wait_recv()
            abuf[k] = pbuf[k] + pe_in[k]
            a_copy(k).start()

    def stage_f(k):
        @pl.when(inner)
        def _():
            a_copy(k).wait_recv()
            fall[sp, k] = abuf[k] + mb_in[k]
            fz_copy(k).start()

        @pl.when(is_end)
        def _():
            fz_copy(k).wait_recv()

        fy_copy(k, sp).start()
        fs_copy(k, sp).start()

    def stage_y(k):
        fy_copy(k, yn).wait_recv()
        gs_copy(k, yn).start()

    def stage_o(k):
        fs_copy(k, sib).wait_recv()
        gs_copy(k, diag).wait_recv()
        r, j = k // per_half, k % per_half
        cols = slice(j * COLS, (j + 1) * COLS)
        for owner in range(4):
            oy, oc = owner // 2, owner % 2
            start = oc * 2 * own_rows + oy * own_rows + r * rows
            out_ref[start:start + rows, cols] = (
                hid_ref[start:start + rows, cols].astype(jnp.float32) + fall[owner, k]).astype(jnp.bfloat16)

    stages = ((stage_a, 0), (stage_f, 2), (stage_y, 4), (stage_o, 6))
    for step in range(chunks + 6):
        for stage, lag in stages:
            if 0 <= step - lag < chunks:
                stage(step - lag)

    for k in range(chunks):
        @pl.when(inner)
        def _():
            a_copy(k).wait_send()
            fz_copy(k).wait_send()

        @pl.when(is_end)
        def _():
            p_copy(k).wait_send()

        fy_copy(k, sp).wait_send()
        fs_copy(k, sp).wait_send()
        gs_copy(k, yn).wait_send()


def combine(acc, stats, hidden, w_out):
    batch, width = acc.shape
    features = w_out.shape[1]
    rows = batch // (4 * HALVES)
    chunks = HALVES * (features // COLS)
    dma = lambda *shape: pltpu.SemaphoreType.DMA(shape)
    f32 = lambda *shape: pltpu.VMEM(shape, jnp.float32)
    vmem, hbm = pl.BlockSpec(memory_space=pltpu.VMEM), pl.BlockSpec(memory_space=pltpu.HBM)
    return pl.pallas_call(
        combine_kernel,
        out_shape=jax.ShapeDtypeStruct((batch, features), jnp.bfloat16),
        in_specs=[vmem, vmem, hbm, hbm],
        out_specs=vmem,
        scratch_shapes=[
            pltpu.VMEM(hidden.shape, jnp.bfloat16),
            pltpu.VMEM(w_out.shape, jnp.bfloat16),
            f32(3, stats.shape[0], batch // 2),
            f32(batch // 2, batch // 2),
            f32(2, HALVES, rows, width),
            f32(HALVES, rows, width),
            f32(HALVES, rows, width),
            pltpu.VMEM((HALVES, rows, width), jnp.bfloat16),
            f32(chunks, rows, COLS),
            f32(chunks, rows, COLS),
            f32(chunks, rows, COLS),
            f32(chunks, rows, COLS),
            f32(4, chunks, rows, COLS),
            pltpu.SemaphoreType.DMA, pltpu.SemaphoreType.DMA, dma(3), dma(3), dma(2 * HALVES), dma(2 * HALVES), dma(HALVES), dma(HALVES),
        ] + [dma(chunks)] * 12,
        compiler_params=pltpu.CompilerParams(collective_id=0, has_side_effects=True, vmem_limit_bytes=int(COMBINE_VMEM * 2**20)),
        name='combine',
    )(acc, stats, hidden, w_out)


def attend_kernel(len_ref, hid_hbm, gain_ref, wq_hbm, wk_hbm, wv_hbm, k_hbm, v_hbm, kout_hbm, vout_hbm, acc_ref, stats_ref,
                  hid, nbuf, wq, wk, wv, kbuf, vbuf, qbuf, nk, nv, statbuf, hid_sem, wq_sem, wk_sem, wv_sem, k_sem, v_sem,
                  ko_sem, vo_sem):
    batch, features = hid.shape
    heads = qbuf.shape[1] // 128
    base = lax.axis_index('sp') * BLOCK
    pieces = k_sem.shape[0]
    seqs = batch // pieces
    piece = seqs * BLOCK * 2
    copy = pltpu.make_async_copy
    quarter = batch // hid_sem.shape[0]
    hid_copies = [copy(hid_hbm.at[pl.ds(i * quarter, quarter), :], hid.at[pl.ds(i * quarter, quarter), :], hid_sem.at[i])
                  for i in range(hid_sem.shape[0])]
    wk_copy, wv_copy = copy(wk_hbm, wk, wk_sem), copy(wv_hbm, wv, wv_sem)
    wide = wq.shape[2]
    wq_copies = [copy(wq_hbm.at[:, pl.ds(i * wide, wide)], wq.at[i], wq_sem.at[i]) for i in range(wq.shape[0])]

    def block_copy(src, dst, sem, i):
        rows = pl.ds(pl.multiple_of(i * piece, piece), piece)
        return copy(src.at[rows, :], dst.at[rows, :], sem.at[i])

    for c in hid_copies + [wk_copy, wv_copy]:
        c.start()

    gain = gain_ref[...].astype(jnp.float32).reshape(1, features)

    def norm_rows(i):
        rows = pl.ds(pl.multiple_of(i * 16, 16), 16)
        h = hid[rows, :].astype(jnp.float32)
        inv_rms = lax.rsqrt(jnp.mean(h * h, axis=-1, keepdims=True) + EPS)
        nbuf[rows, :] = (h * inv_rms * gain).astype(jnp.bfloat16)

    for i, c in enumerate(hid_copies):
        c.wait()
        if i == 0:
            for w in wq_copies:
                w.start()
        if i == 1:
            for j in range(pieces):
                block_copy(k_hbm, kbuf, k_sem, j).start()
                block_copy(v_hbm, vbuf, v_sem, j).start()
        per = quarter // 16
        pl.loop(i * per, (i + 1) * per)(norm_rows)

    for weight, weight_copy, out in ((wk, wk_copy, nk), (wv, wv_copy, nv)):
        weight_copy.wait()
        new = jnp.dot(nbuf[...], weight[...], preferred_element_type=jnp.float32)
        new = new.astype(jnp.bfloat16).astype(jnp.float32)
        for j in range(2):
            out[j] = new[:, j * 128:(j + 1) * 128]

    for i, c in enumerate(wq_copies):
        c.wait()
        query = jnp.dot(nbuf[...], wq[i], preferred_element_type=jnp.float32)
        qbuf[:, i * wide:(i + 1) * wide] = query.astype(jnp.bfloat16).astype(jnp.float32)

    lane = lax.broadcasted_iota(jnp.int32, (8, 128), 1)
    row = lax.broadcasted_iota(jnp.int32, (8, 128), 0)
    slot_pos = base + (lane % 64) // 2
    own_seq = (lane // 64) == (row % 2)
    even = lane % 2 == 0
    pairs = [row // 2 == j for j in range(4)]
    odd_row = row % 2 == 1
    slot_row = lax.broadcasted_iota(jnp.int32, (16, 128), 0) // 2

    def place_new(b):
        at = len_ref[b] - base
        first = jnp.clip(at, 0, BLOCK - 1) // 8
        rows = pl.ds(pl.multiple_of(b * 2 * BLOCK + first * 16, 16), 16)
        here = slot_row == at - first * 8
        for buf, new in ((kbuf, nk), (vbuf, nv)):
            fresh = jnp.where(odd_row, jnp.broadcast_to(new[1, pl.ds(b, 1), :], (8, 128)),
                              jnp.broadcast_to(new[0, pl.ds(b, 1), :], (8, 128)))
            fresh = jnp.concatenate([fresh, fresh], axis=0)
            buf[rows, :] = jnp.where(here, fresh, buf[rows, :].astype(jnp.float32)).astype(jnp.bfloat16)

    def attend_tile(i):
        seq8 = pl.ds(pl.multiple_of(i * 8, 8), 8)
        keys = pl.ds(pl.multiple_of(i * 512, 512), 512)
        q = jnp.concatenate([qbuf[seq8, h * 128:(h + 1) * 128] for h in range(heads)], axis=0).astype(jnp.bfloat16)
        s = lax.dot_general(q, kbuf[keys, :], (((1,), (1,)), ((), ())), preferred_element_type=jnp.float32)
        lens = jnp.full((8, 128), len_ref[i * 8], jnp.int32)
        for j in range(1, 8):
            lens = jnp.where(row == j, len_ref[i * 8 + j], lens)
        valid = jnp.logical_and(own_seq, slot_pos <= lens)
        valids = (jnp.logical_and(valid, even), jnp.logical_and(valid, jnp.logical_not(even)))
        stat = jnp.zeros((8, 128), jnp.float32)
        probs = []
        for h in range(heads):
            part = [s[h * 8:(h + 1) * 8, j * 128:(j + 1) * 128] for j in range(4)]
            score = jnp.where(pairs[0], part[0], jnp.where(pairs[1], part[1], jnp.where(pairs[2], part[2], part[3])))
            ok = valids[h // (heads // 2)]
            score = jnp.where(ok, score * SCALE, NEG_BIG)
            peak = jnp.max(score, axis=1, keepdims=True)
            e = jnp.where(ok, jnp.exp(score - peak), 0.0)
            stat = jnp.where(lane == h, peak, stat)
            stat = jnp.where(lane == heads + h, jnp.sum(e, axis=1, keepdims=True), stat)
            probs.append(jnp.concatenate([jnp.where(pairs[j], e, 0.0) for j in range(4)], axis=1))
        p = jnp.concatenate(probs, axis=0).astype(jnp.bfloat16)
        o = jnp.dot(p, vbuf[keys, :], preferred_element_type=jnp.float32)
        for h in range(heads):
            acc_ref[seq8, h * 128:(h + 1) * 128] = o[h * 8:(h + 1) * 8, :]
        statbuf[seq8, :] = stat

    @pl.loop(0, pieces)
    def _(i):
        block_copy(k_hbm, kbuf, k_sem, i).wait()
        block_copy(v_hbm, vbuf, v_sem, i).wait()

        @pl.loop(0, seqs, unroll=8)
        def _(j):
            place_new(i * seqs + j)

        @pl.loop(0, seqs // 8, unroll=UNROLL)
        def _(j):
            attend_tile(i * (seqs // 8) + j)

        block_copy(kbuf, kout_hbm, ko_sem, i).start()
        block_copy(vbuf, vout_hbm, vo_sem, i).start()

    for i in range(batch // 128):
        stats_ref[:, i * 128:(i + 1) * 128] = statbuf[i * 128:(i + 1) * 128, :].T[0:2 * heads, :]

    for i in range(pieces):
        block_copy(kbuf, kout_hbm, ko_sem, i).wait()
        block_copy(vbuf, vout_hbm, vo_sem, i).wait()


def attend(hidden, lengths, k_cache, v_cache, norm_gain, w_query, w_key, w_value):
    batch, block, kv, dim = k_cache.shape
    features, width = w_query.shape
    slots = batch * block * kv
    bf16 = lambda *shape: pltpu.VMEM(shape, jnp.bfloat16)
    f32 = lambda *shape: pltpu.VMEM(shape, jnp.float32)
    dma = lambda *shape: pltpu.SemaphoreType.DMA(shape)
    vmem, hbm = pl.BlockSpec(memory_space=pltpu.VMEM), pl.BlockSpec(memory_space=pltpu.HBM)
    cache = jax.ShapeDtypeStruct((slots, dim), jnp.bfloat16)
    k_new, v_new, acc, stats = pl.pallas_call(
        attend_kernel,
        out_shape=[cache, cache, jax.ShapeDtypeStruct((batch, width), jnp.float32),
                   jax.ShapeDtypeStruct((2 * width // dim, batch), jnp.float32)],
        in_specs=[pl.BlockSpec(memory_space=pltpu.SMEM), hbm, vmem, hbm, hbm, hbm, hbm, hbm],
        out_specs=[hbm, hbm, vmem, vmem],
        scratch_shapes=[
            bf16(batch, features), bf16(batch, features), bf16(width // 256, features, 256), bf16(features, 256),
            bf16(features, 256), bf16(slots, dim), bf16(slots, dim), f32(batch, width), f32(kv, batch, dim),
            f32(kv, batch, dim), f32(batch, 128),
            dma(4), dma(width // 256), pltpu.SemaphoreType.DMA, pltpu.SemaphoreType.DMA, dma(8), dma(8), dma(8), dma(8),
        ],
        compiler_params=pltpu.CompilerParams(vmem_limit_bytes=int(ATTEND_VMEM * 2**20)),
        name='attend',
    )(lengths, hidden, norm_gain, w_query, w_key, w_value, k_cache.reshape(slots, dim), v_cache.reshape(slots, dim))
    return k_new.reshape(k_cache.shape), v_new.reshape(v_cache.shape), acc, stats


def solution(mesh):
    cache_spec = P('dp', 'sp', 'tp', None)

    def local_step(hidden, lengths, k_cache, v_cache, norm_gain, w_query, w_key, w_value, w_out):
        k_new, v_new, acc, stats = attend(hidden, lengths, k_cache, v_cache, norm_gain, w_query, w_key, w_value)
        return combine(acc, stats, hidden, w_out), k_new, v_new

    return jax.shard_map(
        local_step,
        mesh=mesh,
        in_specs=(P('dp', None), P('dp'), cache_spec, cache_spec, P(None), P(None, 'tp'), P(None, 'tp'), P(None, 'tp'), P('tp', None)),
        out_specs=(P('dp', None), cache_spec, cache_spec),
        check_vma=False,
    )
```

```python
import jax
import jax.numpy as jnp
from jax import lax
from jax.experimental import pallas as pl
from jax.experimental.pallas import tpu as pltpu
from jax.sharding import PartitionSpec as P

EPS = 1e-6
NEG_BIG = -1e30
MESH = pl.DeviceIdType.MESH
HALVES = 2
COLS = 512
GROUP = 4
BLOCK = 32
SCALE = 128 ** -0.5
UNROLL = 8
PIECES = 4
LAGS = (0, 2, 5, 7)
ATTEND_VMEM = 51.5
COMBINE_VMEM = 50


def combine_kernel(acc_ref, stats_ref, hid_hbm, w_hbm, out_ref, hid_ref, w_ref, stat_in, fac_ref, d2d_in, y_out, y_in, obuf, pbuf,
                   pe_in, abuf, mb_in, fall, h_sem, w_sem, st_s, st_r, dd_s, dd_r, yy_s, yy_r, p_s, p_r, a_s, a_r, fz_s, fz_r,
                   fy_s, fy_r, fs_s, fs_r, gs_s, gs_r):
    heads = acc_ref.shape[1] // 128
    rows = obuf.shape[1]
    own_rows = HALVES * rows
    per_half = out_ref.shape[1] // COLS
    chunks = HALVES * per_half
    sp = lax.axis_index('sp')
    z = lax.axis_index('tp')
    y, c = sp // 2, sp % 2
    sib, yn, diag = 2 * y + (1 - c), 2 * (1 - y) + c, 2 * (1 - y) + (1 - c)
    inner = jnp.logical_or(z == 1, z == 2)
    is_end = jnp.logical_or(z == 0, z == 3)
    low = z // 2
    end_z = low * 3
    mid_z = 2 - low
    inner_z = 1 + low

    hid_copy, w_copy = pltpu.make_async_copy(hid_hbm, hid_ref, h_sem), pltpu.make_async_copy(w_hbm, w_ref, w_sem)
    w_copy.start()
    hid_copy.start()

    barrier = pltpu.get_barrier_semaphore()
    for peer in (sib, yn, diag):
        pl.semaphore_signal(barrier, inc=1, device_id={'sp': peer}, device_id_type=MESH)

    @pl.when(inner)
    def _():
        pl.semaphore_signal(barrier, inc=1, device_id={'tp': end_z}, device_id_type=MESH)
        pl.semaphore_signal(barrier, inc=1, device_id={'tp': mid_z}, device_id_type=MESH)
        pl.semaphore_wait(barrier, 5)

    @pl.when(is_end)
    def _():
        pl.semaphore_signal(barrier, inc=1, device_id={'tp': inner_z}, device_id_type=MESH)
        pl.semaphore_wait(barrier, 4)

    def remote(src, dst, send, recv, **where):
        return pltpu.make_async_remote_copy(src_ref=src, dst_ref=dst, send_sem=send, recv_sem=recv, device_id=where,
                                            device_id_type=MESH)

    def stat_copy(i, peer):
        lanes = pl.ds(pl.multiple_of((peer % 2) * 2 * own_rows, 128), 2 * own_rows)
        return remote(stats_ref.at[:, lanes], stat_in.at[i], st_s.at[i], st_r.at[i], sp=peer)

    stat_copies = [stat_copy(i, peer) for i, peer in enumerate((sib, yn, diag))]
    for copy in stat_copies:
        copy.start()

    def d2d_copy(t, r):
        plane = (1 - y) if t == 0 else y
        start = pl.multiple_of((1 - c) * 2 * own_rows + plane * own_rows + r * rows, rows)
        return remote(acc_ref.at[pl.ds(start, rows), :], d2d_in.at[t, r], dd_s.at[2 * r + t], dd_r.at[2 * r + t], sp=sib)

    d2d_copies = [[d2d_copy(t, r) for r in range(HALVES)] for t in range(2)]
    for r in range(HALVES):
        for t in range(2):
            d2d_copies[t][r].start()

    for copy in stat_copies:
        copy.wait()
    lanes = pl.ds(pl.multiple_of(c * 2 * own_rows, 128), 2 * own_rows)
    peaks = [stats_ref[0:heads, lanes]] + [stat_in[i, 0:heads, :] for i in range(3)]
    sums = [stats_ref[heads:2 * heads, lanes]] + [stat_in[i, heads:2 * heads, :] for i in range(3)]
    top = jnp.maximum(jnp.maximum(peaks[0], peaks[1]), jnp.maximum(peaks[2], peaks[3]))
    weights = [jnp.exp(peak - top) for peak in peaks]
    total = sums[0] * weights[0] + sums[1] * weights[1] + (sums[2] * weights[2] + sums[3] * weights[3])
    factors = jnp.concatenate(
        [weights[0] / total, weights[1] / total, jnp.zeros((2 * own_rows - 2 * heads, 2 * own_rows), jnp.float32)], axis=0)
    fac_ref[...] = factors.T

    def combined(t, r, j):
        plane = (1 - y) if t == 0 else y
        base = pl.multiple_of(plane * own_rows + r * rows, rows)
        start = pl.multiple_of(c * 2 * own_rows + base, rows)
        cols = slice(j * 128, (j + 1) * 128)
        mine = acc_ref[pl.ds(start, rows), cols] * fac_ref[pl.ds(base, rows), j:j + 1]
        return mine + d2d_in[t, r, :, cols] * fac_ref[pl.ds(base, rows), heads + j:heads + j + 1]

    def y_copy(r):
        return remote(y_out.at[r], y_in.at[r], yy_s.at[r], yy_r.at[r], sp=yn)

    y_copies = [y_copy(r) for r in range(HALVES)]
    for r in range(HALVES):
        d2d_copies[0][r].wait()
        for j in range(heads):
            y_out[r, :, j * 128:(j + 1) * 128] = combined(0, r, j)
        y_copies[r].start()

    def p_copy(k):
        return remote(pbuf.at[k], pe_in.at[k], p_s.at[k], p_r.at[k], tp=inner_z)

    def a_copy(k):
        return remote(abuf.at[k], mb_in.at[k], a_s.at[k], a_r.at[k], tp=mid_z)

    def fz_copy(k):
        return remote(fall.at[sp, k], fall.at[sp, k], fz_s.at[k], fz_r.at[k], tp=end_z)

    def fy_copy(k, owner):
        return remote(fall.at[owner, k], fall.at[owner, k], fy_s.at[k], fy_r.at[k], sp=yn)

    def fs_copy(k, owner):
        return remote(fall.at[owner, k], fall.at[owner, k], fs_s.at[k], fs_r.at[k], sp=sib)

    def gs_copy(k, owner):
        return remote(fall.at[owner, k], fall.at[owner, k], gs_s.at[k], gs_r.at[k], sp=sib)

    def merge(r):
        d2d_copies[1][r].wait()
        y_copies[r].wait()
        for j in range(heads):
            obuf[r, :, j * 128:(j + 1) * 128] = (combined(1, r, j) + y_in[r, :, j * 128:(j + 1) * 128]).astype(jnp.bfloat16)

    def project(first):
        for k in range(first, first + GROUP):
            cols = slice(k % per_half * COLS, (k % per_half + 1) * COLS)
            pbuf[k] = jnp.dot(obuf[k // per_half], w_ref[:, cols], preferred_element_type=jnp.float32)

        @pl.when(is_end)
        def _():
            for k in range(first, first + GROUP):
                p_copy(k).start()

    def stage_a(k):
        @pl.when(inner)
        def _():
            p_copy(k).wait_recv()
            abuf[k] = pbuf[k] + pe_in[k]
            a_copy(k).start()

    def stage_f(k):
        @pl.when(inner)
        def _():
            a_copy(k).wait_recv()
            fall[sp, k] = abuf[k] + mb_in[k]
            fz_copy(k).start()

        @pl.when(is_end)
        def _():
            fz_copy(k).wait_recv()

        fy_copy(k, sp).start()
        fs_copy(k, sp).start()

    def stage_y(k):
        fy_copy(k, yn).wait_recv()
        gs_copy(k, yn).start()

    def stage_o(k):
        fs_copy(k, sib).wait_recv()
        gs_copy(k, diag).wait_recv()
        r, j = k // per_half, k % per_half
        cols = slice(j * COLS, (j + 1) * COLS)
        for owner in range(4):
            oy, oc = owner // 2, owner % 2
            start = oc * 2 * own_rows + oy * own_rows + r * rows
            out_ref[start:start + rows, cols] = (
                hid_ref[start:start + rows, cols].astype(jnp.float32) + fall[owner, k]).astype(jnp.bfloat16)

    w_copy.wait()
    merge(0)
    for first in range(0, per_half, GROUP):
        project(first)
    hid_copy.wait()
    later = {0: [(merge, 1)]}
    for i, first in enumerate(range(per_half, chunks, GROUP)):
        later[1 + i] = [(project, first)]
    stages = tuple(zip((stage_a, stage_f, stage_y, stage_o), LAGS))
    for step in range(chunks + LAGS[-1]):
        for stage, lag in stages:
            if 0 <= step - lag < chunks:
                stage(step - lag)
        for task, which in later.get(step, ()):
            task(which)

    for k in range(chunks):
        @pl.when(inner)
        def _():
            a_copy(k).wait_send()
            fz_copy(k).wait_send()

        @pl.when(is_end)
        def _():
            p_copy(k).wait_send()

        fy_copy(k, sp).wait_send()
        fs_copy(k, sp).wait_send()
        gs_copy(k, yn).wait_send()


def combine(acc, stats, hidden, w_out):
    batch, width = acc.shape
    features = w_out.shape[1]
    rows = batch // (4 * HALVES)
    chunks = HALVES * (features // COLS)
    dma = lambda *shape: pltpu.SemaphoreType.DMA(shape)
    f32 = lambda *shape: pltpu.VMEM(shape, jnp.float32)
    vmem, hbm = pl.BlockSpec(memory_space=pltpu.VMEM), pl.BlockSpec(memory_space=pltpu.HBM)
    return pl.pallas_call(
        combine_kernel,
        out_shape=jax.ShapeDtypeStruct((batch, features), jnp.bfloat16),
        in_specs=[vmem, vmem, hbm, hbm],
        out_specs=vmem,
        scratch_shapes=[
            pltpu.VMEM(hidden.shape, jnp.bfloat16),
            pltpu.VMEM(w_out.shape, jnp.bfloat16),
            f32(3, stats.shape[0], batch // 2),
            f32(batch // 2, batch // 2),
            f32(2, HALVES, rows, width),
            f32(HALVES, rows, width),
            f32(HALVES, rows, width),
            pltpu.VMEM((HALVES, rows, width), jnp.bfloat16),
            f32(chunks, rows, COLS),
            f32(chunks, rows, COLS),
            f32(chunks, rows, COLS),
            f32(chunks, rows, COLS),
            f32(4, chunks, rows, COLS),
            pltpu.SemaphoreType.DMA, pltpu.SemaphoreType.DMA, dma(3), dma(3), dma(2 * HALVES), dma(2 * HALVES), dma(HALVES), dma(HALVES),
        ] + [dma(chunks)] * 12,
        compiler_params=pltpu.CompilerParams(collective_id=0, has_side_effects=True, vmem_limit_bytes=int(COMBINE_VMEM * 2**20)),
        name='combine',
    )(acc, stats, hidden, w_out)


def attend_kernel(len_hbm, hid_hbm, gain_hbm, wq_hbm, wk_hbm, wv_hbm, k_hbm, v_hbm, kout_hbm, vout_hbm, acc_ref, stats_ref,
                  hid, nbuf, wq, wk, wv, kbuf, vbuf, qbuf, nk, nv, statbuf, len_ref, gain_ref, hid_sem, wq_sem, wk_sem, wv_sem, k_sem, v_sem,
                  ko_sem, vo_sem, len_sem, gain_sem):
    batch, features = hid.shape
    heads = qbuf.shape[1] // 128
    base = lax.axis_index('sp') * BLOCK
    pieces = k_sem.shape[0]
    seqs = batch // pieces
    piece = seqs * BLOCK * 2
    copy = pltpu.make_async_copy
    quarter = batch // hid_sem.shape[0]
    hid_copies = [copy(hid_hbm.at[pl.ds(i * quarter, quarter), :], hid.at[pl.ds(i * quarter, quarter), :], hid_sem.at[i])
                  for i in range(hid_sem.shape[0])]
    wk_copy, wv_copy = copy(wk_hbm, wk, wk_sem), copy(wv_hbm, wv, wv_sem)
    wide, deep = 256, features // wq_sem.shape[0]
    wq_copies = [copy(wq_hbm.at[pl.ds(i * deep, deep), :], wq.at[pl.ds(i * deep, deep), :], wq_sem.at[i])
                 for i in range(wq_sem.shape[0])]

    def block_copy(src, dst, sem, i):
        rows = pl.ds(pl.multiple_of(i * piece, piece), piece)
        return copy(src.at[rows, :], dst.at[rows, :], sem.at[i])

    gain_copy, len_copy = copy(gain_hbm, gain_ref, gain_sem), copy(len_hbm, len_ref, len_sem)
    for c in [gain_copy, len_copy] + hid_copies + [wk_copy, wv_copy]:
        c.start()

    def norm_rows(i):
        rows = pl.ds(pl.multiple_of(i * 16, 16), 16)
        h = hid[rows, :].astype(jnp.float32)
        gain = gain_ref[...].astype(jnp.float32).reshape(1, features)
        inv_rms = lax.rsqrt(jnp.mean(h * h, axis=-1, keepdims=True) + EPS)
        nbuf[rows, :] = (h * inv_rms * gain).astype(jnp.bfloat16)

    for i, c in enumerate(hid_copies):
        c.wait()
        if i == 0:
            gain_copy.wait()
            len_copy.wait()
            for j in range(pieces):
                block_copy(k_hbm, kbuf, k_sem, j).start()
                block_copy(v_hbm, vbuf, v_sem, j).start()
        if i == 2:
            for w in wq_copies:
                w.start()
        per = quarter // 16
        pl.loop(i * per, (i + 1) * per)(norm_rows)

    for weight, weight_copy, out in ((wk, wk_copy, nk), (wv, wv_copy, nv)):
        weight_copy.wait()
        new = jnp.dot(nbuf[...], weight[...], preferred_element_type=jnp.float32)
        new = new.astype(jnp.bfloat16).astype(jnp.float32)
        for j in range(2):
            out[j] = new[:, j * 128:(j + 1) * 128]

    lane = lax.broadcasted_iota(jnp.int32, (8, 128), 1)
    row = lax.broadcasted_iota(jnp.int32, (8, 128), 0)
    slot_pos = base + (lane % 64) // 2
    own_seq = (lane // 64) == (row % 2)
    even = lane % 2 == 0
    pairs = [row // 2 == j for j in range(4)]
    odd_row = row % 2 == 1
    slot_row = lax.broadcasted_iota(jnp.int32, (16, 128), 0) // 2

    def place_new(g):
        group = pl.ds(pl.multiple_of(g * 8, 8), 8)
        news = [(new[0, group, :], new[1, group, :]) for new in (nk, nv)]
        spots = []
        for j in range(8):
            b = g * 8 + j
            at = len_ref[b] - base
            first = jnp.clip(at, 0, BLOCK - 1) // 8
            rows = pl.ds(pl.multiple_of(b * 2 * BLOCK + first * 16, 16), 16)
            spots.append((rows, slot_row == at - first * 8))
        olds = [(kbuf[rows, :], vbuf[rows, :]) for rows, _ in spots]
        for j, (rows, here) in enumerate(spots):
            for buf, (low, high), old in zip((kbuf, vbuf), news, olds[j]):
                fresh = jnp.where(odd_row, jnp.broadcast_to(high[j:j + 1], (8, 128)), jnp.broadcast_to(low[j:j + 1], (8, 128)))
                fresh = jnp.concatenate([fresh, fresh], axis=0)
                buf[rows, :] = jnp.where(here, fresh, old.astype(jnp.float32)).astype(jnp.bfloat16)

    def scores(i):
        seq8 = pl.ds(pl.multiple_of(i * 8, 8), 8)
        keys = pl.ds(pl.multiple_of(i * 512, 512), 512)
        q = jnp.concatenate([qbuf[seq8, h * 128:(h + 1) * 128] for h in range(heads)], axis=0).astype(jnp.bfloat16)
        s = lax.dot_general(q, kbuf[keys, :], (((1,), (1,)), ((), ())), preferred_element_type=jnp.float32)
        out = []
        for h in range(heads):
            part = [s[h * 8:(h + 1) * 8, j * 128:(j + 1) * 128] for j in range(4)]
            out.append(jnp.where(pairs[0], part[0], jnp.where(pairs[1], part[1], jnp.where(pairs[2], part[2], part[3]))))
        return out

    def softmax(i, score_list):
        seq8 = pl.ds(pl.multiple_of(i * 8, 8), 8)
        lens = jnp.full((8, 128), len_ref[i * 8], jnp.int32)
        for j in range(1, 8):
            lens = jnp.where(row == j, len_ref[i * 8 + j], lens)
        valid = jnp.logical_and(own_seq, slot_pos <= lens)
        valids = (jnp.logical_and(valid, even), jnp.logical_and(valid, jnp.logical_not(even)))
        oks = [valids[h // (heads // 2)] for h in range(heads)]
        masked = [jnp.where(ok, score * SCALE, NEG_BIG) for ok, score in zip(oks, score_list)]
        peaks = [jnp.max(score, axis=1, keepdims=True) for score in masked]
        exps = [jnp.where(ok, jnp.exp(score - peak), 0.0) for ok, score, peak in zip(oks, masked, peaks)]
        sums = [jnp.sum(e, axis=1, keepdims=True) for e in exps]
        stat = jnp.zeros((8, 128), jnp.float32)
        for h in range(heads):
            stat = jnp.where(lane == h, peaks[h], jnp.where(lane == heads + h, sums[h], stat))
        statbuf[seq8, :] = stat
        probs = [jnp.concatenate([jnp.where(pairs[j], e, 0.0) for j in range(4)], axis=1) for e in exps]
        return jnp.concatenate(probs, axis=0).astype(jnp.bfloat16)

    def values(i, p):
        seq8 = pl.ds(pl.multiple_of(i * 8, 8), 8)
        keys = pl.ds(pl.multiple_of(i * 512, 512), 512)
        o = jnp.dot(p, vbuf[keys, :], preferred_element_type=jnp.float32)
        for h in range(heads):
            acc_ref[seq8, h * 128:(h + 1) * 128] = o[h * 8:(h + 1) * 8, :]

    per_piece = seqs // 8

    @pl.loop(0, pieces)
    def _(i):
        block_copy(k_hbm, kbuf, k_sem, i).wait()
        block_copy(v_hbm, vbuf, v_sem, i).wait()

        @pl.loop(0, per_piece)
        def _(j):
            place_new(i * per_piece + j)

    for c in wq_copies:
        c.wait()
    for i in range(wq.shape[1] // wide):
        query = jnp.dot(nbuf[...], wq[:, i * wide:(i + 1) * wide], preferred_element_type=jnp.float32)
        qbuf[:, i * wide:(i + 1) * wide] = query.astype(jnp.bfloat16).astype(jnp.float32)

    for i in range(pieces):
        block_copy(kbuf, kout_hbm, ko_sem, i).start()
        block_copy(vbuf, vout_hbm, vo_sem, i).start()

    @pl.loop(0, pieces)
    def _(i):
        @pl.loop(0, per_piece, step=UNROLL)
        def _(j):
            tiles = [i * per_piece + j + u for u in range(UNROLL)]
            score_lists = [scores(t) for t in tiles]
            prob_list = [softmax(t, score_list) for t, score_list in zip(tiles, score_lists)]
            for t, p in zip(tiles, prob_list):
                values(t, p)

    for i in range(batch // 128):
        stats_ref[:, i * 128:(i + 1) * 128] = statbuf[i * 128:(i + 1) * 128, :].T[0:2 * heads, :]

    for i in range(pieces):
        block_copy(kbuf, kout_hbm, ko_sem, i).wait()
        block_copy(vbuf, vout_hbm, vo_sem, i).wait()


def attend(hidden, lengths, k_cache, v_cache, norm_gain, w_query, w_key, w_value):
    batch, block, kv, dim = k_cache.shape
    features, width = w_query.shape
    slots = batch * block * kv
    bf16 = lambda *shape: pltpu.VMEM(shape, jnp.bfloat16)
    f32 = lambda *shape: pltpu.VMEM(shape, jnp.float32)
    dma, one = lambda *shape: pltpu.SemaphoreType.DMA(shape), pltpu.SemaphoreType.DMA
    hbm, vmem = pl.BlockSpec(memory_space=pltpu.HBM), pl.BlockSpec(memory_space=pltpu.VMEM)
    cache = jax.ShapeDtypeStruct((slots, dim), jnp.bfloat16)
    k_new, v_new, acc, stats = pl.pallas_call(
        attend_kernel,
        out_shape=[cache, cache, jax.ShapeDtypeStruct((batch, width), jnp.float32),
                   jax.ShapeDtypeStruct((2 * width // dim, batch), jnp.float32)],
        in_specs=[hbm] * 8,
        out_specs=[hbm, hbm, vmem, vmem],
        scratch_shapes=[
            bf16(batch, features), bf16(batch, features), bf16(features, width), bf16(features, 256),
            bf16(features, 256), bf16(slots, dim), bf16(slots, dim), f32(batch, width), f32(kv, batch, dim),
            f32(kv, batch, dim), f32(batch, 128), pltpu.SMEM((batch,), jnp.int32), bf16(features),
            dma(4), dma(width // 256), one, one, dma(PIECES), dma(PIECES), dma(PIECES), dma(PIECES), one, one,
        ],
        compiler_params=pltpu.CompilerParams(vmem_limit_bytes=int(ATTEND_VMEM * 2**20)),
        name='attend',
    )(lengths, hidden, norm_gain, w_query, w_key, w_value, k_cache.reshape(slots, dim), v_cache.reshape(slots, dim))
    return k_new.reshape(k_cache.shape), v_new.reshape(v_cache.shape), acc, stats


def solution(mesh):
    cache_spec = P('dp', 'sp', 'tp', None)

    def local_step(hidden, lengths, k_cache, v_cache, norm_gain, w_query, w_key, w_value, w_out):
        k_new, v_new, acc, stats = attend(hidden, lengths, k_cache, v_cache, norm_gain, w_query, w_key, w_value)
        return combine(acc, stats, hidden, w_out), k_new, v_new

    return jax.shard_map(
        local_step,
        mesh=mesh,
        in_specs=(P('dp', None), P('dp'), cache_spec, cache_spec, P(None), P(None, 'tp'), P(None, 'tp'), P(None, 'tp'), P('tp', None)),
        out_specs=(P('dp', None), cache_spec, cache_spec),
        check_vma=False,
    )
```

```python
import jax
import jax.numpy as jnp
from jax import lax
from jax.experimental import pallas as pl
from jax.experimental.pallas import tpu as pltpu
from jax.sharding import PartitionSpec as P

EPS = 1e-6
NEG_BIG = -1e30
MESH = pl.DeviceIdType.MESH
HALVES = 4
EARLY = 2
COLS = 1024
GROUP = 4
BLOCK = 32
SCALE = 128 ** -0.5
UNROLL = 8
PIECES = 4
LAGS = (0, 3, 6, 8)
ATTEND_VMEM = 51.5
COMBINE_VMEM = 50


def combine_kernel(acc_ref, stats_ref, hid_hbm, w_hbm, out_ref, hid_ref, w_ref, stat_in, fac_ref, d2d_in, y_out, y_in, obuf, pbuf,
                   pe_in, abuf, mb_in, fall, h_sem, w_sem, st_s, st_r, dd_s, dd_r, yy_s, yy_r, p_s, p_r, a_s, a_r, fz_s, fz_r,
                   fy_s, fy_r, fs_s, fs_r, gs_s, gs_r):
    heads = acc_ref.shape[1] // 128
    rows = obuf.shape[1]
    own_rows = HALVES * rows
    per_half = out_ref.shape[1] // COLS
    chunks = HALVES * per_half
    sp = lax.axis_index('sp')
    z = lax.axis_index('tp')
    y, c = sp // 2, sp % 2
    sib, yn, diag = 2 * y + (1 - c), 2 * (1 - y) + c, 2 * (1 - y) + (1 - c)
    inner = jnp.logical_or(z == 1, z == 2)
    is_end = jnp.logical_or(z == 0, z == 3)
    low = z // 2
    end_z = low * 3
    mid_z = 2 - low
    inner_z = 1 + low

    hid_copy, w_copy = pltpu.make_async_copy(hid_hbm, hid_ref, h_sem), pltpu.make_async_copy(w_hbm, w_ref, w_sem)
    w_copy.start()
    hid_copy.start()

    barrier = pltpu.get_barrier_semaphore()
    for peer in (sib, yn, diag):
        pl.semaphore_signal(barrier, inc=1, device_id={'sp': peer}, device_id_type=MESH)

    @pl.when(inner)
    def _():
        pl.semaphore_signal(barrier, inc=1, device_id={'tp': end_z}, device_id_type=MESH)
        pl.semaphore_signal(barrier, inc=1, device_id={'tp': mid_z}, device_id_type=MESH)
        pl.semaphore_wait(barrier, 5)

    @pl.when(is_end)
    def _():
        pl.semaphore_signal(barrier, inc=1, device_id={'tp': inner_z}, device_id_type=MESH)
        pl.semaphore_wait(barrier, 4)

    def remote(src, dst, send, recv, **where):
        return pltpu.make_async_remote_copy(src_ref=src, dst_ref=dst, send_sem=send, recv_sem=recv, device_id=where,
                                            device_id_type=MESH)

    def stat_copy(i, peer):
        lanes = pl.ds(pl.multiple_of((peer % 2) * 2 * own_rows, 128), 2 * own_rows)
        return remote(stats_ref.at[:, lanes], stat_in.at[i], st_s.at[i], st_r.at[i], sp=peer)

    stat_copies = [stat_copy(i, peer) for i, peer in enumerate((sib, yn, diag))]
    for copy in stat_copies:
        copy.start()

    def d2d_copy(t, r):
        plane = (1 - y) if t == 0 else y
        start = pl.multiple_of((1 - c) * 2 * own_rows + plane * own_rows + r * rows, rows)
        return remote(acc_ref.at[pl.ds(start, rows), :], d2d_in.at[t, r], dd_s.at[2 * r + t], dd_r.at[2 * r + t], sp=sib)

    d2d_copies = [[d2d_copy(t, r) for r in range(HALVES)] for t in range(2)]
    for t in range(2):
        for r in range(HALVES):
            d2d_copies[t][r].start()

    lanes = pl.ds(pl.multiple_of(c * 2 * own_rows, 128), 2 * own_rows)
    stat_copies[0].wait()
    peaks = [stats_ref[0:heads, lanes], stat_in[0, 0:heads, :]]
    sums = [stats_ref[heads:2 * heads, lanes], stat_in[0, heads:2 * heads, :]]
    chip_top = jnp.maximum(peaks[0], peaks[1])
    unused = jnp.zeros((2 * own_rows - 2 * heads, 2 * own_rows), jnp.float32)
    fac_ref[0] = jnp.concatenate([jnp.exp(peaks[0] - chip_top), jnp.exp(peaks[1] - chip_top), unused], axis=0).T

    def combined(t, r, j):
        plane = (1 - y) if t == 0 else y
        base = pl.multiple_of(plane * own_rows + r * rows, rows)
        start = pl.multiple_of(c * 2 * own_rows + base, rows)
        cols = slice(j * 128, (j + 1) * 128)
        mine = acc_ref[pl.ds(start, rows), cols] * fac_ref[0, pl.ds(base, rows), j:j + 1]
        return mine + d2d_in[t, r, :, cols] * fac_ref[0, pl.ds(base, rows), heads + j:heads + j + 1]

    def y_copy(r):
        return remote(y_out.at[r], y_in.at[r], yy_s.at[r], yy_r.at[r], sp=yn)

    y_copies = [y_copy(r) for r in range(HALVES)]
    for r in range(HALVES):
        d2d_copies[0][r].wait()
        for j in range(heads):
            y_out[r, :, j * 128:(j + 1) * 128] = combined(0, r, j)
        y_copies[r].start()

    for copy in stat_copies[1:]:
        copy.wait()
    peaks += [stat_in[i, 0:heads, :] for i in (1, 2)]
    sums += [stat_in[i, heads:2 * heads, :] for i in (1, 2)]
    far_top = jnp.maximum(peaks[2], peaks[3])
    top = jnp.maximum(chip_top, far_top)
    parts = [one_sum * jnp.exp(peak - top) for one_sum, peak in zip(sums, peaks)]
    total = parts[0] + parts[1] + (parts[2] + parts[3])
    fac_ref[1] = jnp.concatenate([jnp.exp(chip_top - top) / total, jnp.exp(far_top - top) / total, unused], axis=0).T

    def p_copy(k):
        return remote(pbuf.at[k], pe_in.at[k], p_s.at[k], p_r.at[k], tp=inner_z)

    def a_copy(k):
        return remote(abuf.at[k], mb_in.at[k], a_s.at[k], a_r.at[k], tp=mid_z)

    def fz_copy(k):
        return remote(fall.at[sp, k], fall.at[sp, k], fz_s.at[k], fz_r.at[k], tp=end_z)

    def fy_copy(k, owner):
        return remote(fall.at[owner, k], fall.at[owner, k], fy_s.at[k], fy_r.at[k], sp=yn)

    def fs_copy(k, owner):
        return remote(fall.at[owner, k], fall.at[owner, k], fs_s.at[k], fs_r.at[k], sp=sib)

    def gs_copy(k, owner):
        return remote(fall.at[owner, k], fall.at[owner, k], gs_s.at[k], gs_r.at[k], sp=sib)

    def merge(r):
        d2d_copies[1][r].wait()
        y_copies[r].wait()
        base = pl.multiple_of(y * own_rows + r * rows, rows)
        for j in range(heads):
            near = combined(1, r, j) * fac_ref[1, pl.ds(base, rows), j:j + 1]
            far = y_in[r, :, j * 128:(j + 1) * 128] * fac_ref[1, pl.ds(base, rows), heads + j:heads + j + 1]
            obuf[r, :, j * 128:(j + 1) * 128] = (near + far).astype(jnp.bfloat16)

    def project(first):
        for k in range(first, first + GROUP):
            cols = slice(k % per_half * COLS, (k % per_half + 1) * COLS)
            pbuf[k] = jnp.dot(obuf[k // per_half], w_ref[:, cols], preferred_element_type=jnp.float32)

        @pl.when(is_end)
        def _():
            for k in range(first, first + GROUP):
                p_copy(k).start()

    def stage_a(k):
        @pl.when(inner)
        def _():
            p_copy(k).wait_recv()
            abuf[k] = pbuf[k] + pe_in[k]
            a_copy(k).start()

    def stage_f(k):
        @pl.when(inner)
        def _():
            a_copy(k).wait_recv()
            fall[sp, k] = abuf[k] + mb_in[k]
            fz_copy(k).start()

        @pl.when(is_end)
        def _():
            fz_copy(k).wait_recv()

        fy_copy(k, sp).start()
        fs_copy(k, sp).start()

    def stage_y(k):
        fy_copy(k, yn).wait_recv()
        gs_copy(k, yn).start()

    def stage_o(k):
        fs_copy(k, sib).wait_recv()
        gs_copy(k, diag).wait_recv()
        r, j = k // per_half, k % per_half
        cols = slice(j * COLS, (j + 1) * COLS)
        for owner in range(4):
            oy, oc = owner // 2, owner % 2
            start = oc * 2 * own_rows + oy * own_rows + r * rows
            out_ref[start:start + rows, cols] = (
                hid_ref[start:start + rows, cols].astype(jnp.float32) + fall[owner, k]).astype(jnp.bfloat16)

    w_copy.wait()
    for r in range(EARLY):
        merge(r)
        for first in range(r * per_half, (r + 1) * per_half, GROUP):
            project(first)
    hid_copy.wait()
    later = {}
    for r in range(EARLY, HALVES):
        later.setdefault(r - EARLY, []).append((merge, r))
        for i, first in enumerate(range(r * per_half, (r + 1) * per_half, GROUP)):
            later.setdefault(r - EARLY + i + (HALVES == 2), []).append((project, first))
    stages = tuple(zip((stage_a, stage_f, stage_y, stage_o), LAGS))
    for step in range(chunks + LAGS[-1]):
        for stage, lag in stages:
            if 0 <= step - lag < chunks:
                stage(step - lag)
        for task, which in later.get(step, ()):
            task(which)

    for k in range(chunks):
        @pl.when(inner)
        def _():
            a_copy(k).wait_send()
            fz_copy(k).wait_send()

        @pl.when(is_end)
        def _():
            p_copy(k).wait_send()

        fy_copy(k, sp).wait_send()
        fs_copy(k, sp).wait_send()
        gs_copy(k, yn).wait_send()


def combine(acc, stats, hidden, w_out):
    batch, width = acc.shape
    features = w_out.shape[1]
    rows = batch // (4 * HALVES)
    chunks = HALVES * (features // COLS)
    dma = lambda *shape: pltpu.SemaphoreType.DMA(shape)
    f32 = lambda *shape: pltpu.VMEM(shape, jnp.float32)
    vmem, hbm = pl.BlockSpec(memory_space=pltpu.VMEM), pl.BlockSpec(memory_space=pltpu.HBM)
    return pl.pallas_call(
        combine_kernel,
        out_shape=jax.ShapeDtypeStruct((batch, features), jnp.bfloat16),
        in_specs=[vmem, vmem, hbm, hbm],
        out_specs=vmem,
        scratch_shapes=[
            pltpu.VMEM(hidden.shape, jnp.bfloat16),
            pltpu.VMEM(w_out.shape, jnp.bfloat16),
            f32(3, stats.shape[0], batch // 2),
            f32(2, batch // 2, batch // 2),
            f32(2, HALVES, rows, width),
            f32(HALVES, rows, width),
            f32(HALVES, rows, width),
            pltpu.VMEM((HALVES, rows, width), jnp.bfloat16),
            f32(chunks, rows, COLS),
            f32(chunks, rows, COLS),
            f32(chunks, rows, COLS),
            f32(chunks, rows, COLS),
            f32(4, chunks, rows, COLS),
            pltpu.SemaphoreType.DMA, pltpu.SemaphoreType.DMA, dma(3), dma(3), dma(2 * HALVES), dma(2 * HALVES), dma(HALVES), dma(HALVES),
        ] + [dma(chunks)] * 12,
        compiler_params=pltpu.CompilerParams(collective_id=0, has_side_effects=True, vmem_limit_bytes=int(COMBINE_VMEM * 2**20)),
        name='combine',
    )(acc, stats, hidden, w_out)


def attend_kernel(len_hbm, hid_hbm, gain_hbm, wq_hbm, wk_hbm, wv_hbm, k_hbm, v_hbm, kout_hbm, vout_hbm, acc_ref, stats_ref,
                  hid, nbuf, wq, wk, wv, kbuf, vbuf, qbuf, nk, nv, statbuf, len_ref, gain_ref, hid_sem, wq_sem, wk_sem, wv_sem, k_sem, v_sem,
                  ko_sem, vo_sem, len_sem, gain_sem):
    batch, features = hid.shape
    heads = qbuf.shape[1] // 128
    base = lax.axis_index('sp') * BLOCK
    pieces = k_sem.shape[0]
    seqs = batch // pieces
    piece = seqs * BLOCK * 2
    copy = pltpu.make_async_copy
    quarter = batch // hid_sem.shape[0]
    hid_copies = [copy(hid_hbm.at[pl.ds(i * quarter, quarter), :], hid.at[pl.ds(i * quarter, quarter), :], hid_sem.at[i])
                  for i in range(hid_sem.shape[0])]
    wk_copy, wv_copy = copy(wk_hbm, wk, wk_sem), copy(wv_hbm, wv, wv_sem)
    wide, deep = 256, features // wq_sem.shape[0]
    wq_copies = [copy(wq_hbm.at[pl.ds(i * deep, deep), :], wq.at[pl.ds(i * deep, deep), :], wq_sem.at[i])
                 for i in range(wq_sem.shape[0])]

    def block_copy(src, dst, sem, i):
        rows = pl.ds(pl.multiple_of(i * piece, piece), piece)
        return copy(src.at[rows, :], dst.at[rows, :], sem.at[i])

    gain_copy, len_copy = copy(gain_hbm, gain_ref, gain_sem), copy(len_hbm, len_ref, len_sem)
    for c in [gain_copy, len_copy] + hid_copies + [wk_copy, wv_copy]:
        c.start()

    def norm_rows(i):
        rows = pl.ds(pl.multiple_of(i * 16, 16), 16)
        h = hid[rows, :].astype(jnp.float32)
        gain = gain_ref[...].astype(jnp.float32).reshape(1, features)
        inv_rms = lax.rsqrt(jnp.mean(h * h, axis=-1, keepdims=True) + EPS)
        nbuf[rows, :] = (h * inv_rms * gain).astype(jnp.bfloat16)

    for i, c in enumerate(hid_copies):
        c.wait()
        if i == 0:
            gain_copy.wait()
            len_copy.wait()
            for j in range(pieces):
                block_copy(k_hbm, kbuf, k_sem, j).start()
                block_copy(v_hbm, vbuf, v_sem, j).start()
        if i == 2:
            for w in wq_copies:
                w.start()
        per = quarter // 16
        pl.loop(i * per, (i + 1) * per)(norm_rows)

    for weight, weight_copy, out in ((wk, wk_copy, nk), (wv, wv_copy, nv)):
        weight_copy.wait()
        new = jnp.dot(nbuf[...], weight[...], preferred_element_type=jnp.float32)
        new = new.astype(jnp.bfloat16).astype(jnp.float32)
        for j in range(2):
            out[j] = new[:, j * 128:(j + 1) * 128]

    lane = lax.broadcasted_iota(jnp.int32, (8, 128), 1)
    row = lax.broadcasted_iota(jnp.int32, (8, 128), 0)
    slot_pos = base + (lane % 64) // 2
    own_seq = (lane // 64) == (row % 2)
    even = lane % 2 == 0
    pairs = [row // 2 == j for j in range(4)]
    odd_row = row % 2 == 1
    slot_row = lax.broadcasted_iota(jnp.int32, (16, 128), 0) // 2

    def place_new(g):
        group = pl.ds(pl.multiple_of(g * 8, 8), 8)
        news = [(new[0, group, :], new[1, group, :]) for new in (nk, nv)]
        spots = []
        for j in range(8):
            b = g * 8 + j
            at = len_ref[b] - base
            first = jnp.clip(at, 0, BLOCK - 1) // 8
            rows = pl.ds(pl.multiple_of(b * 2 * BLOCK + first * 16, 16), 16)
            spots.append((rows, slot_row == at - first * 8))
        olds = [(kbuf[rows, :], vbuf[rows, :]) for rows, _ in spots]
        for j, (rows, here) in enumerate(spots):
            for buf, (low, high), old in zip((kbuf, vbuf), news, olds[j]):
                fresh = jnp.where(odd_row, jnp.broadcast_to(high[j:j + 1], (8, 128)), jnp.broadcast_to(low[j:j + 1], (8, 128)))
                fresh = jnp.concatenate([fresh, fresh], axis=0)
                buf[rows, :] = jnp.where(here, fresh, old.astype(jnp.float32)).astype(jnp.bfloat16)

    def scores(i):
        seq8 = pl.ds(pl.multiple_of(i * 8, 8), 8)
        keys = pl.ds(pl.multiple_of(i * 512, 512), 512)
        q = jnp.concatenate([qbuf[seq8, h * 128:(h + 1) * 128] for h in range(heads)], axis=0).astype(jnp.bfloat16)
        s = lax.dot_general(q, kbuf[keys, :], (((1,), (1,)), ((), ())), preferred_element_type=jnp.float32)
        out = []
        for h in range(heads):
            part = [s[h * 8:(h + 1) * 8, j * 128:(j + 1) * 128] for j in range(4)]
            out.append(jnp.where(pairs[0], part[0], jnp.where(pairs[1], part[1], jnp.where(pairs[2], part[2], part[3]))))
        return out

    def softmax(i, score_list):
        seq8 = pl.ds(pl.multiple_of(i * 8, 8), 8)
        lens = jnp.full((8, 128), len_ref[i * 8], jnp.int32)
        for j in range(1, 8):
            lens = jnp.where(row == j, len_ref[i * 8 + j], lens)
        valid = jnp.logical_and(own_seq, slot_pos <= lens)
        valids = (jnp.logical_and(valid, even), jnp.logical_and(valid, jnp.logical_not(even)))
        oks = [valids[h // (heads // 2)] for h in range(heads)]
        masked = [jnp.where(ok, score * SCALE, NEG_BIG) for ok, score in zip(oks, score_list)]
        peaks = [jnp.max(score, axis=1, keepdims=True) for score in masked]
        exps = [jnp.where(ok, jnp.exp(score - peak), 0.0) for ok, score, peak in zip(oks, masked, peaks)]
        sums = [jnp.sum(e, axis=1, keepdims=True) for e in exps]
        stat = jnp.zeros((8, 128), jnp.float32)
        for h in range(heads):
            stat = jnp.where(lane == h, peaks[h], jnp.where(lane == heads + h, sums[h], stat))
        statbuf[seq8, :] = stat
        probs = [jnp.concatenate([jnp.where(pairs[j], e, 0.0) for j in range(4)], axis=1) for e in exps]
        return jnp.concatenate(probs, axis=0).astype(jnp.bfloat16)

    def values(i, p):
        seq8 = pl.ds(pl.multiple_of(i * 8, 8), 8)
        keys = pl.ds(pl.multiple_of(i * 512, 512), 512)
        o = jnp.dot(p, vbuf[keys, :], preferred_element_type=jnp.float32)
        for h in range(heads):
            acc_ref[seq8, h * 128:(h + 1) * 128] = o[h * 8:(h + 1) * 8, :]

    per_piece = seqs // 8

    @pl.loop(0, pieces)
    def _(i):
        block_copy(k_hbm, kbuf, k_sem, i).wait()
        block_copy(v_hbm, vbuf, v_sem, i).wait()

        @pl.loop(0, per_piece)
        def _(j):
            place_new(i * per_piece + j)

    for c in wq_copies:
        c.wait()
    for i in range(wq.shape[1] // wide):
        query = jnp.dot(nbuf[...], wq[:, i * wide:(i + 1) * wide], preferred_element_type=jnp.float32)
        qbuf[:, i * wide:(i + 1) * wide] = query.astype(jnp.bfloat16).astype(jnp.float32)

    for i in range(pieces):
        block_copy(kbuf, kout_hbm, ko_sem, i).start()
        block_copy(vbuf, vout_hbm, vo_sem, i).start()

    @pl.loop(0, pieces)
    def _(i):
        @pl.loop(0, per_piece, step=UNROLL)
        def _(j):
            tiles = [i * per_piece + j + u for u in range(UNROLL)]
            score_lists = [scores(t) for t in tiles]
            prob_list = [softmax(t, score_list) for t, score_list in zip(tiles, score_lists)]
            for t, p in zip(tiles, prob_list):
                values(t, p)

    for i in range(batch // 128):
        stats_ref[:, i * 128:(i + 1) * 128] = statbuf[i * 128:(i + 1) * 128, :].T[0:2 * heads, :]

    for i in range(pieces):
        block_copy(kbuf, kout_hbm, ko_sem, i).wait()
        block_copy(vbuf, vout_hbm, vo_sem, i).wait()


def attend(hidden, lengths, k_cache, v_cache, norm_gain, w_query, w_key, w_value):
    batch, block, kv, dim = k_cache.shape
    features, width = w_query.shape
    slots = batch * block * kv
    bf16 = lambda *shape: pltpu.VMEM(shape, jnp.bfloat16)
    f32 = lambda *shape: pltpu.VMEM(shape, jnp.float32)
    dma, one = lambda *shape: pltpu.SemaphoreType.DMA(shape), pltpu.SemaphoreType.DMA
    hbm, vmem = pl.BlockSpec(memory_space=pltpu.HBM), pl.BlockSpec(memory_space=pltpu.VMEM)
    cache = jax.ShapeDtypeStruct((slots, dim), jnp.bfloat16)
    k_new, v_new, acc, stats = pl.pallas_call(
        attend_kernel,
        out_shape=[cache, cache, jax.ShapeDtypeStruct((batch, width), jnp.float32),
                   jax.ShapeDtypeStruct((2 * width // dim, batch), jnp.float32)],
        in_specs=[hbm] * 8,
        out_specs=[hbm, hbm, vmem, vmem],
        scratch_shapes=[
            bf16(batch, features), bf16(batch, features), bf16(features, width), bf16(features, 256),
            bf16(features, 256), bf16(slots, dim), bf16(slots, dim), f32(batch, width), f32(kv, batch, dim),
            f32(kv, batch, dim), f32(batch, 128), pltpu.SMEM((batch,), jnp.int32), bf16(features),
            dma(4), dma(width // 256), one, one, dma(PIECES), dma(PIECES), dma(PIECES), dma(PIECES), one, one,
        ],
        compiler_params=pltpu.CompilerParams(vmem_limit_bytes=int(ATTEND_VMEM * 2**20)),
        name='attend',
    )(lengths, hidden, norm_gain, w_query, w_key, w_value, k_cache.reshape(slots, dim), v_cache.reshape(slots, dim))
    return k_new.reshape(k_cache.shape), v_new.reshape(v_cache.shape), acc, stats


def solution(mesh):
    cache_spec = P('dp', 'sp', 'tp', None)

    def local_step(hidden, lengths, k_cache, v_cache, norm_gain, w_query, w_key, w_value, w_out):
        k_new, v_new, acc, stats = attend(hidden, lengths, k_cache, v_cache, norm_gain, w_query, w_key, w_value)
        return combine(acc, stats, hidden, w_out), k_new, v_new

    return jax.shard_map(
        local_step,
        mesh=mesh,
        in_specs=(P('dp', None), P('dp'), cache_spec, cache_spec, P(None), P(None, 'tp'), P(None, 'tp'), P(None, 'tp'), P('tp', None)),
        out_specs=(P('dp', None), cache_spec, cache_spec),
        check_vma=False,
    )
```

```python
import jax
import jax.numpy as jnp
from jax import lax
from jax.experimental import pallas as pl
from jax.experimental.pallas import tpu as pltpu
from jax.sharding import PartitionSpec as P

EPS = 1e-6
NEG_BIG = -1e30
MESH = pl.DeviceIdType.MESH
HALVES = 4
EARLY = 2
COLS = 1024
GROUP = 4
BLOCK = 32
SCALE = 128 ** -0.5
UNROLL = 8
PIECES = 4
LAGS = (0, 3, 6, 8)
ATTEND_VMEM = 51.5
COMBINE_VMEM = 50


def combine_kernel(acc_ref, stats_ref, hid_hbm, w_hbm, out_ref, hid_ref, w_ref, stat_in, fac_ref, d2d_in, y_out, y_in, obuf, pbuf,
                   pe_in, abuf, mb_in, fall, h_sem, w_sem, st_s, st_r, dd_s, dd_r, yy_s, yy_r, p_s, p_r, a_s, a_r, fz_s, fz_r,
                   fy_s, fy_r, fs_s, fs_r, gs_s, gs_r):
    heads = acc_ref.shape[1] // 128
    rows = obuf.shape[1]
    own_rows = HALVES * rows
    per_half = out_ref.shape[1] // COLS
    chunks = HALVES * per_half
    sp = lax.axis_index('sp')
    z = lax.axis_index('tp')
    y, c = sp // 2, sp % 2
    sib, yn, diag = 2 * y + (1 - c), 2 * (1 - y) + c, 2 * (1 - y) + (1 - c)
    inner = jnp.logical_or(z == 1, z == 2)
    is_end = jnp.logical_or(z == 0, z == 3)
    low = z // 2
    end_z = low * 3
    mid_z = 2 - low
    inner_z = 1 + low

    hid_copy, w_copy = pltpu.make_async_copy(hid_hbm, hid_ref, h_sem), pltpu.make_async_copy(w_hbm, w_ref, w_sem)
    w_copy.start()
    hid_copy.start()

    barrier = pltpu.get_barrier_semaphore()
    for peer in (sib, yn, diag):
        pl.semaphore_signal(barrier, inc=1, device_id={'sp': peer}, device_id_type=MESH)

    @pl.when(inner)
    def _():
        pl.semaphore_signal(barrier, inc=1, device_id={'tp': end_z}, device_id_type=MESH)
        pl.semaphore_signal(barrier, inc=1, device_id={'tp': mid_z}, device_id_type=MESH)
        pl.semaphore_wait(barrier, 5)

    @pl.when(is_end)
    def _():
        pl.semaphore_signal(barrier, inc=1, device_id={'tp': inner_z}, device_id_type=MESH)
        pl.semaphore_wait(barrier, 4)

    def remote(src, dst, send, recv, **where):
        return pltpu.make_async_remote_copy(src_ref=src, dst_ref=dst, send_sem=send, recv_sem=recv, device_id=where,
                                            device_id_type=MESH)

    def stat_copy(i, peer):
        lanes = pl.ds(pl.multiple_of((peer % 2) * 2 * own_rows, 128), 2 * own_rows)
        return remote(stats_ref.at[:, lanes], stat_in.at[i], st_s.at[i], st_r.at[i], sp=peer)

    stat_copies = [stat_copy(i, peer) for i, peer in enumerate((sib, yn, diag))]
    for copy in stat_copies:
        copy.start()

    def d2d_copy(t, r):
        plane = (1 - y) if t == 0 else y
        start = pl.multiple_of((1 - c) * 2 * own_rows + plane * own_rows + r * rows, rows)
        return remote(acc_ref.at[pl.ds(start, rows), :], d2d_in.at[t, r], dd_s.at[2 * r + t], dd_r.at[2 * r + t], sp=sib)

    d2d_copies = [[d2d_copy(t, r) for r in range(HALVES)] for t in range(2)]
    for t in range(2):
        for r in range(HALVES):
            d2d_copies[t][r].start()

    lanes = pl.ds(pl.multiple_of(c * 2 * own_rows, 128), 2 * own_rows)
    stat_copies[0].wait()
    peaks = [stats_ref[0:heads, lanes], stat_in[0, 0:heads, :]]
    sums = [stats_ref[heads:2 * heads, lanes], stat_in[0, heads:2 * heads, :]]
    chip_top = jnp.maximum(peaks[0], peaks[1])
    unused = jnp.zeros((2 * own_rows - 2 * heads, 2 * own_rows), jnp.float32)
    fac_ref[0] = jnp.concatenate([jnp.exp(peaks[0] - chip_top), jnp.exp(peaks[1] - chip_top), unused], axis=0).T

    def combined(t, r, j):
        plane = (1 - y) if t == 0 else y
        base = pl.multiple_of(plane * own_rows + r * rows, rows)
        start = pl.multiple_of(c * 2 * own_rows + base, rows)
        cols = slice(j * 128, (j + 1) * 128)
        mine = acc_ref[pl.ds(start, rows), cols] * fac_ref[0, pl.ds(base, rows), j:j + 1]
        return mine + d2d_in[t, r, :, cols] * fac_ref[0, pl.ds(base, rows), heads + j:heads + j + 1]

    def y_copy(r):
        return remote(y_out.at[r], y_in.at[r], yy_s.at[r], yy_r.at[r], sp=yn)

    y_copies = [y_copy(r) for r in range(HALVES)]
    for r in range(HALVES):
        d2d_copies[0][r].wait()
        for j in range(heads):
            y_out[r, :, j * 128:(j + 1) * 128] = combined(0, r, j)
        y_copies[r].start()

    for copy in stat_copies[1:]:
        copy.wait()
    peaks += [stat_in[i, 0:heads, :] for i in (1, 2)]
    sums += [stat_in[i, heads:2 * heads, :] for i in (1, 2)]
    far_top = jnp.maximum(peaks[2], peaks[3])
    top = jnp.maximum(chip_top, far_top)
    parts = [one_sum * jnp.exp(peak - top) for one_sum, peak in zip(sums, peaks)]
    total = parts[0] + parts[1] + (parts[2] + parts[3])
    fac_ref[1] = jnp.concatenate([jnp.exp(chip_top - top) / total, jnp.exp(far_top - top) / total, unused], axis=0).T

    def p_copy(k):
        return remote(pbuf.at[k], pe_in.at[k], p_s, p_r.at[k], tp=inner_z)

    def a_copy(k):
        return remote(abuf.at[k], mb_in.at[k], a_s, a_r.at[k], tp=mid_z)

    def fz_copy(k):
        return remote(fall.at[sp, k], fall.at[sp, k], fz_s, fz_r.at[k], tp=end_z)

    def fy_copy(k, owner):
        return remote(fall.at[owner, k], fall.at[owner, k], fy_s, fy_r.at[k], sp=yn)

    def fs_copy(k, owner):
        return remote(fall.at[owner, k], fall.at[owner, k], fs_s, fs_r.at[k], sp=sib)

    def gs_copy(k, owner):
        return remote(fall.at[owner, k], fall.at[owner, k], gs_s, gs_r.at[k], sp=sib)

    def merge(r):
        d2d_copies[1][r].wait()
        y_copies[r].wait()
        base = pl.multiple_of(y * own_rows + r * rows, rows)
        for j in range(heads):
            near = combined(1, r, j) * fac_ref[1, pl.ds(base, rows), j:j + 1]
            far = y_in[r, :, j * 128:(j + 1) * 128] * fac_ref[1, pl.ds(base, rows), heads + j:heads + j + 1]
            obuf[r, :, j * 128:(j + 1) * 128] = (near + far).astype(jnp.bfloat16)

    def project(first):
        for k in range(first, first + GROUP):
            cols = slice(k % per_half * COLS, (k % per_half + 1) * COLS)
            pbuf[k] = jnp.dot(obuf[k // per_half], w_ref[:, cols], preferred_element_type=jnp.float32)

        @pl.when(is_end)
        def _():
            for k in range(first, first + GROUP):
                p_copy(k).start()

    def stage_a(k):
        @pl.when(inner)
        def _():
            p_copy(k).wait_recv()
            abuf[k] = pbuf[k] + pe_in[k]
            a_copy(k).start()

    def stage_f(k):
        @pl.when(inner)
        def _():
            a_copy(k).wait_recv()
            fall[sp, k] = abuf[k] + mb_in[k]
            fz_copy(k).start()

        @pl.when(is_end)
        def _():
            fz_copy(k).wait_recv()

        fy_copy(k, sp).start()
        fs_copy(k, sp).start()

    def stage_y(k):
        fy_copy(k, yn).wait_recv()
        gs_copy(k, yn).start()

    def stage_o(k):
        fs_copy(k, sib).wait_recv()
        gs_copy(k, diag).wait_recv()
        r, j = k // per_half, k % per_half
        cols = slice(j * COLS, (j + 1) * COLS)
        for owner in range(4):
            oy, oc = owner // 2, owner % 2
            start = oc * 2 * own_rows + oy * own_rows + r * rows
            out_ref[start:start + rows, cols] = (
                hid_ref[start:start + rows, cols].astype(jnp.float32) + fall[owner, k]).astype(jnp.bfloat16)

    w_copy.wait()
    for r in range(EARLY):
        merge(r)
        for first in range(r * per_half, (r + 1) * per_half, GROUP):
            project(first)
    hid_copy.wait()
    later = {}
    for r in range(EARLY, HALVES):
        later.setdefault(r - EARLY, []).append((merge, r))
        for i, first in enumerate(range(r * per_half, (r + 1) * per_half, GROUP)):
            later.setdefault(r - EARLY + i + (HALVES == 2), []).append((project, first))
    stages = tuple(zip((stage_a, stage_f, stage_y, stage_o), LAGS))
    for step in range(chunks + LAGS[-1]):
        for stage, lag in stages:
            if 0 <= step - lag < chunks:
                stage(step - lag)
        for task, which in later.get(step, ()):
            task(which)

    def all_sent(src, send, **where):
        remote(src, src, send, fs_r.at[0], **where).wait_send()

    @pl.when(inner)
    def _():
        all_sent(abuf, a_s, tp=mid_z)
        all_sent(fall.at[sp], fz_s, tp=end_z)

    @pl.when(is_end)
    def _():
        all_sent(pbuf, p_s, tp=inner_z)

    all_sent(fall.at[sp], fy_s, sp=yn)
    all_sent(fall.at[sp], fs_s, sp=sib)
    all_sent(fall.at[yn], gs_s, sp=sib)


def combine(acc, stats, hidden, w_out):
    batch, width = acc.shape
    features = w_out.shape[1]
    rows = batch // (4 * HALVES)
    chunks = HALVES * (features // COLS)
    dma = lambda *shape: pltpu.SemaphoreType.DMA(shape)
    f32 = lambda *shape: pltpu.VMEM(shape, jnp.float32)
    vmem, hbm = pl.BlockSpec(memory_space=pltpu.VMEM), pl.BlockSpec(memory_space=pltpu.HBM)
    return pl.pallas_call(
        combine_kernel,
        out_shape=jax.ShapeDtypeStruct((batch, features), jnp.bfloat16),
        in_specs=[vmem, vmem, hbm, hbm],
        out_specs=vmem,
        scratch_shapes=[
            pltpu.VMEM(hidden.shape, jnp.bfloat16),
            pltpu.VMEM(w_out.shape, jnp.bfloat16),
            f32(3, stats.shape[0], batch // 2),
            f32(2, batch // 2, batch // 2),
            f32(2, HALVES, rows, width),
            f32(HALVES, rows, width),
            f32(HALVES, rows, width),
            pltpu.VMEM((HALVES, rows, width), jnp.bfloat16),
            f32(chunks, rows, COLS),
            f32(chunks, rows, COLS),
            f32(chunks, rows, COLS),
            f32(chunks, rows, COLS),
            f32(4, chunks, rows, COLS),
            pltpu.SemaphoreType.DMA, pltpu.SemaphoreType.DMA, dma(3), dma(3), dma(2 * HALVES), dma(2 * HALVES), dma(HALVES), dma(HALVES),
        ] + [pltpu.SemaphoreType.DMA, dma(chunks)] * 6,
        compiler_params=pltpu.CompilerParams(collective_id=0, has_side_effects=True, vmem_limit_bytes=int(COMBINE_VMEM * 2**20)),
        name='combine',
    )(acc, stats, hidden, w_out)


def attend_kernel(len_hbm, hid_hbm, gain_hbm, wq_hbm, wk_hbm, wv_hbm, k_hbm, v_hbm, kout_hbm, vout_hbm, acc_ref, stats_ref,
                  hid, nbuf, wq, wk, wv, kbuf, vbuf, qbuf, nk, nv, statbuf, len_ref, gain_ref, hid_sem, wq_sem, wk_sem, wv_sem, k_sem, v_sem,
                  ko_sem, vo_sem, len_sem, gain_sem):
    batch, features = hid.shape
    heads = qbuf.shape[1] // 128
    base = lax.axis_index('sp') * BLOCK
    pieces = k_sem.shape[0]
    seqs = batch // pieces
    piece = seqs * BLOCK * 2
    copy = pltpu.make_async_copy
    quarter = batch // hid_sem.shape[0]
    hid_copies = [copy(hid_hbm.at[pl.ds(i * quarter, quarter), :], hid.at[pl.ds(i * quarter, quarter), :], hid_sem.at[i])
                  for i in range(hid_sem.shape[0])]
    wk_copy, wv_copy = copy(wk_hbm, wk, wk_sem), copy(wv_hbm, wv, wv_sem)
    wide, deep = 256, features // wq_sem.shape[0]
    wq_copies = [copy(wq_hbm.at[pl.ds(i * deep, deep), :], wq.at[pl.ds(i * deep, deep), :], wq_sem.at[i])
                 for i in range(wq_sem.shape[0])]

    def block_copy(src, dst, sem, i):
        rows = pl.ds(pl.multiple_of(i * piece, piece), piece)
        return copy(src.at[rows, :], dst.at[rows, :], sem.at[i])

    gain_copy, len_copy = copy(gain_hbm, gain_ref, gain_sem), copy(len_hbm, len_ref, len_sem)
    for c in [gain_copy, len_copy] + hid_copies + [wk_copy, wv_copy]:
        c.start()

    def norm_rows(i):
        rows = pl.ds(pl.multiple_of(i * 16, 16), 16)
        h = hid[rows, :].astype(jnp.float32)
        gain = gain_ref[...].astype(jnp.float32).reshape(1, features)
        inv_rms = lax.rsqrt(jnp.mean(h * h, axis=-1, keepdims=True) + EPS)
        nbuf[rows, :] = (h * inv_rms * gain).astype(jnp.bfloat16)

    for i, c in enumerate(hid_copies):
        c.wait()
        if i == 0:
            gain_copy.wait()
            len_copy.wait()
            for j in range(pieces):
                block_copy(k_hbm, kbuf, k_sem, j).start()
                block_copy(v_hbm, vbuf, v_sem, j).start()
        if i == 2:
            for w in wq_copies:
                w.start()
        per = quarter // 16
        pl.loop(i * per, (i + 1) * per)(norm_rows)

    for weight, weight_copy, out in ((wk, wk_copy, nk), (wv, wv_copy, nv)):
        weight_copy.wait()
        new = jnp.dot(nbuf[...], weight[...], preferred_element_type=jnp.float32)
        new = new.astype(jnp.bfloat16).astype(jnp.float32)
        for j in range(2):
            out[j] = new[:, j * 128:(j + 1) * 128]

    lane = lax.broadcasted_iota(jnp.int32, (8, 128), 1)
    row = lax.broadcasted_iota(jnp.int32, (8, 128), 0)
    slot_pos = base + (lane % 64) // 2
    own_seq = (lane // 64) == (row % 2)
    even = lane % 2 == 0
    pairs = [row // 2 == j for j in range(4)]
    odd_row = row % 2 == 1
    slot_row = lax.broadcasted_iota(jnp.int32, (16, 128), 0) // 2

    def place_new(g):
        group = pl.ds(pl.multiple_of(g * 8, 8), 8)
        news = [(new[0, group, :], new[1, group, :]) for new in (nk, nv)]
        spots = []
        for j in range(8):
            b = g * 8 + j
            at = len_ref[b] - base
            first = jnp.clip(at, 0, BLOCK - 1) // 8
            rows = pl.ds(pl.multiple_of(b * 2 * BLOCK + first * 16, 16), 16)
            spots.append((rows, slot_row == at - first * 8))
        olds = [(kbuf[rows, :], vbuf[rows, :]) for rows, _ in spots]
        for j, (rows, here) in enumerate(spots):
            for buf, (low, high), old in zip((kbuf, vbuf), news, olds[j]):
                fresh = jnp.where(odd_row, jnp.broadcast_to(high[j:j + 1], (8, 128)), jnp.broadcast_to(low[j:j + 1], (8, 128)))
                fresh = jnp.concatenate([fresh, fresh], axis=0)
                buf[rows, :] = jnp.where(here, fresh, old.astype(jnp.float32)).astype(jnp.bfloat16)

    def scores(i):
        seq8 = pl.ds(pl.multiple_of(i * 8, 8), 8)
        keys = pl.ds(pl.multiple_of(i * 512, 512), 512)
        q = jnp.concatenate([qbuf[seq8, h * 128:(h + 1) * 128] for h in range(heads)], axis=0).astype(jnp.bfloat16)
        s = lax.dot_general(q, kbuf[keys, :], (((1,), (1,)), ((), ())), preferred_element_type=jnp.float32)
        out = []
        for h in range(heads):
            part = [s[h * 8:(h + 1) * 8, j * 128:(j + 1) * 128] for j in range(4)]
            out.append(jnp.where(pairs[0], part[0], jnp.where(pairs[1], part[1], jnp.where(pairs[2], part[2], part[3]))))
        return out

    def softmax(i, score_list):
        seq8 = pl.ds(pl.multiple_of(i * 8, 8), 8)
        lens = jnp.full((8, 128), len_ref[i * 8], jnp.int32)
        for j in range(1, 8):
            lens = jnp.where(row == j, len_ref[i * 8 + j], lens)
        valid = jnp.logical_and(own_seq, slot_pos <= lens)
        valids = (jnp.logical_and(valid, even), jnp.logical_and(valid, jnp.logical_not(even)))
        oks = [valids[h // (heads // 2)] for h in range(heads)]
        masked = [jnp.where(ok, score * SCALE, NEG_BIG) for ok, score in zip(oks, score_list)]
        peaks = [jnp.max(score, axis=1, keepdims=True) for score in masked]
        exps = [jnp.where(ok, jnp.exp(score - peak), 0.0) for ok, score, peak in zip(oks, masked, peaks)]
        sums = [jnp.sum(e, axis=1, keepdims=True) for e in exps]
        stat = jnp.zeros((8, 128), jnp.float32)
        for h in range(heads):
            stat = jnp.where(lane == h, peaks[h], jnp.where(lane == heads + h, sums[h], stat))
        statbuf[seq8, :] = stat
        probs = [jnp.concatenate([jnp.where(pairs[j], e, 0.0) for j in range(4)], axis=1) for e in exps]
        return jnp.concatenate(probs, axis=0).astype(jnp.bfloat16)

    def values(i, p):
        seq8 = pl.ds(pl.multiple_of(i * 8, 8), 8)
        keys = pl.ds(pl.multiple_of(i * 512, 512), 512)
        o = jnp.dot(p, vbuf[keys, :], preferred_element_type=jnp.float32)
        for h in range(heads):
            acc_ref[seq8, h * 128:(h + 1) * 128] = o[h * 8:(h + 1) * 8, :]

    per_piece = seqs // 8

    @pl.loop(0, pieces)
    def _(i):
        block_copy(k_hbm, kbuf, k_sem, i).wait()
        block_copy(v_hbm, vbuf, v_sem, i).wait()

        @pl.loop(0, per_piece)
        def _(j):
            place_new(i * per_piece + j)

    for c in wq_copies:
        c.wait()
    for i in range(wq.shape[1] // wide):
        query = jnp.dot(nbuf[...], wq[:, i * wide:(i + 1) * wide], preferred_element_type=jnp.float32)
        qbuf[:, i * wide:(i + 1) * wide] = query.astype(jnp.bfloat16).astype(jnp.float32)

    for i in range(pieces):
        block_copy(kbuf, kout_hbm, ko_sem, i).start()
        block_copy(vbuf, vout_hbm, vo_sem, i).start()

    @pl.loop(0, pieces)
    def _(i):
        @pl.loop(0, per_piece, step=UNROLL)
        def _(j):
            tiles = [i * per_piece + j + u for u in range(UNROLL)]
            score_lists = [scores(t) for t in tiles]
            prob_list = [softmax(t, score_list) for t, score_list in zip(tiles, score_lists)]
            for t, p in zip(tiles, prob_list):
                values(t, p)

    for i in range(batch // 128):
        stats_ref[:, i * 128:(i + 1) * 128] = statbuf[i * 128:(i + 1) * 128, :].T[0:2 * heads, :]

    for i in range(pieces):
        block_copy(kbuf, kout_hbm, ko_sem, i).wait()
        block_copy(vbuf, vout_hbm, vo_sem, i).wait()


def attend(hidden, lengths, k_cache, v_cache, norm_gain, w_query, w_key, w_value):
    batch, block, kv, dim = k_cache.shape
    features, width = w_query.shape
    slots = batch * block * kv
    bf16 = lambda *shape: pltpu.VMEM(shape, jnp.bfloat16)
    f32 = lambda *shape: pltpu.VMEM(shape, jnp.float32)
    dma, one = lambda *shape: pltpu.SemaphoreType.DMA(shape), pltpu.SemaphoreType.DMA
    hbm, vmem = pl.BlockSpec(memory_space=pltpu.HBM), pl.BlockSpec(memory_space=pltpu.VMEM)
    cache = jax.ShapeDtypeStruct((slots, dim), jnp.bfloat16)
    k_new, v_new, acc, stats = pl.pallas_call(
        attend_kernel,
        out_shape=[cache, cache, jax.ShapeDtypeStruct((batch, width), jnp.float32),
                   jax.ShapeDtypeStruct((2 * width // dim, batch), jnp.float32)],
        in_specs=[hbm] * 8,
        out_specs=[hbm, hbm, vmem, vmem],
        scratch_shapes=[
            bf16(batch, features), bf16(batch, features), bf16(features, width), bf16(features, 256),
            bf16(features, 256), bf16(slots, dim), bf16(slots, dim), f32(batch, width), f32(kv, batch, dim),
            f32(kv, batch, dim), f32(batch, 128), pltpu.SMEM((batch,), jnp.int32), bf16(features),
            dma(4), dma(width // 256), one, one, dma(PIECES), dma(PIECES), dma(PIECES), dma(PIECES), one, one,
        ],
        compiler_params=pltpu.CompilerParams(vmem_limit_bytes=int(ATTEND_VMEM * 2**20)),
        name='attend',
    )(pltpu.with_memory_space_constraint(lengths, pltpu.HBM), hidden, pltpu.with_memory_space_constraint(norm_gain, pltpu.HBM), w_query, w_key, w_value, k_cache.reshape(slots, dim), v_cache.reshape(slots, dim))
    return k_new.reshape(k_cache.shape), v_new.reshape(v_cache.shape), acc, stats


def solution(mesh):
    cache_spec = P('dp', 'sp', 'tp', None)

    def local_step(hidden, lengths, k_cache, v_cache, norm_gain, w_query, w_key, w_value, w_out):
        k_new, v_new, acc, stats = attend(hidden, lengths, k_cache, v_cache, norm_gain, w_query, w_key, w_value)
        return combine(acc, stats, hidden, w_out), k_new, v_new

    return jax.shard_map(
        local_step,
        mesh=mesh,
        in_specs=(P('dp', None), P('dp'), cache_spec, cache_spec, P(None), P(None, 'tp'), P(None, 'tp'), P(None, 'tp'), P('tp', None)),
        out_specs=(P('dp', None), cache_spec, cache_spec),
        check_vma=False,
    )
```

```python
import jax
import jax.numpy as jnp
from jax import lax
from jax.experimental import pallas as pl
from jax.experimental.pallas import tpu as pltpu
from jax.sharding import PartitionSpec as P

EPS = 1e-6
NEG_BIG = -1e30
MESH = pl.DeviceIdType.MESH
HALVES = 4
EARLY = 1
COLS = 1024
GROUP = 4
BLOCK = 32
SCALE = 128 ** -0.5
UNROLL = 16
PIECES = 2
LAGS = (0, 3, 6, 8)
ATTEND_VMEM = 51.5
COMBINE_VMEM = 50


def combine_kernel(acc_ref, stats_ref, hid_hbm, w_hbm, out_ref, hid_ref, w_ref, stat_in, fac_ref, d2d_in, y_out, y_in, obuf, pbuf,
                   pe_in, abuf, mb_in, fall, h_sem, w_sem, st_s, st_r, dd_s, dd_r, yy_s, yy_r, p_s, p_r, a_s, a_r, fz_s, fz_r,
                   fy_s, fy_r, fs_s, fs_r, gs_s, gs_r):
    heads = acc_ref.shape[1] // 128
    rows = obuf.shape[1]
    own_rows = HALVES * rows
    per_half = out_ref.shape[1] // COLS
    chunks = HALVES * per_half
    sp = lax.axis_index('sp')
    z = lax.axis_index('tp')
    y, c = sp // 2, sp % 2
    sib, yn, diag = 2 * y + (1 - c), 2 * (1 - y) + c, 2 * (1 - y) + (1 - c)
    inner = jnp.logical_or(z == 1, z == 2)
    is_end = jnp.logical_or(z == 0, z == 3)
    low = z // 2
    end_z = low * 3
    mid_z = 2 - low
    inner_z = 1 + low

    hid_copy, w_copy = pltpu.make_async_copy(hid_hbm, hid_ref, h_sem), pltpu.make_async_copy(w_hbm, w_ref, w_sem)
    w_copy.start()
    hid_copy.start()

    barrier = pltpu.get_barrier_semaphore()
    for peer in (sib, yn, diag):
        pl.semaphore_signal(barrier, inc=1, device_id={'sp': peer}, device_id_type=MESH)

    @pl.when(inner)
    def _():
        pl.semaphore_signal(barrier, inc=1, device_id={'tp': end_z}, device_id_type=MESH)
        pl.semaphore_signal(barrier, inc=1, device_id={'tp': mid_z}, device_id_type=MESH)
        pl.semaphore_wait(barrier, 5)

    @pl.when(is_end)
    def _():
        pl.semaphore_signal(barrier, inc=1, device_id={'tp': inner_z}, device_id_type=MESH)
        pl.semaphore_wait(barrier, 4)

    def remote(src, dst, send, recv, **where):
        return pltpu.make_async_remote_copy(src_ref=src, dst_ref=dst, send_sem=send, recv_sem=recv, device_id=where,
                                            device_id_type=MESH)

    def stat_copy(i, peer):
        lanes = pl.ds(pl.multiple_of((peer % 2) * 2 * own_rows, 128), 2 * own_rows)
        return remote(stats_ref.at[:, lanes], stat_in.at[i], st_s.at[i], st_r.at[i], sp=peer)

    stat_copies = [stat_copy(i, peer) for i, peer in enumerate((sib, yn, diag))]
    for copy in stat_copies:
        copy.start()

    def d2d_copy(t, r):
        plane = (1 - y) if t == 0 else y
        start = pl.multiple_of((1 - c) * 2 * own_rows + plane * own_rows + r * rows, rows)
        return remote(acc_ref.at[pl.ds(start, rows), :], d2d_in.at[t, r], dd_s.at[2 * r + t], dd_r.at[2 * r + t], sp=sib)

    d2d_copies = [[d2d_copy(t, r) for r in range(HALVES)] for t in range(2)]
    for t in range(2):
        for r in range(HALVES):
            d2d_copies[t][r].start()

    lanes = pl.ds(pl.multiple_of(c * 2 * own_rows, 128), 2 * own_rows)
    stat_copies[0].wait()
    peaks = [stats_ref[0:heads, lanes], stat_in[0, 0:heads, :]]
    sums = [stats_ref[heads:2 * heads, lanes], stat_in[0, heads:2 * heads, :]]
    chip_top = jnp.maximum(peaks[0], peaks[1])
    unused = jnp.zeros((2 * own_rows - 2 * heads, 2 * own_rows), jnp.float32)
    fac_ref[0] = jnp.concatenate([jnp.exp(peaks[0] - chip_top), jnp.exp(peaks[1] - chip_top), unused], axis=0).T

    def combined(t, r, j):
        plane = (1 - y) if t == 0 else y
        base = pl.multiple_of(plane * own_rows + r * rows, rows)
        start = pl.multiple_of(c * 2 * own_rows + base, rows)
        cols = slice(j * 128, (j + 1) * 128)
        mine = acc_ref[pl.ds(start, rows), cols] * fac_ref[0, pl.ds(base, rows), j:j + 1]
        return mine + d2d_in[t, r, :, cols] * fac_ref[0, pl.ds(base, rows), heads + j:heads + j + 1]

    def y_copy(r):
        return remote(y_out.at[r], y_in.at[r], yy_s.at[r], yy_r.at[r], sp=yn)

    y_copies = [y_copy(r) for r in range(HALVES)]
    for r in range(HALVES):
        d2d_copies[0][r].wait()
        for j in range(heads):
            y_out[r, :, j * 128:(j + 1) * 128] = combined(0, r, j)
        y_copies[r].start()

    for copy in stat_copies[1:]:
        copy.wait()
    peaks += [stat_in[i, 0:heads, :] for i in (1, 2)]
    sums += [stat_in[i, heads:2 * heads, :] for i in (1, 2)]
    far_top = jnp.maximum(peaks[2], peaks[3])
    top = jnp.maximum(chip_top, far_top)
    parts = [one_sum * jnp.exp(peak - top) for one_sum, peak in zip(sums, peaks)]
    total = parts[0] + parts[1] + (parts[2] + parts[3])
    fac_ref[1] = jnp.concatenate([jnp.exp(chip_top - top) / total, jnp.exp(far_top - top) / total, unused], axis=0).T

    def p_copy(k):
        return remote(pbuf.at[k], pe_in.at[k], p_s, p_r.at[k], tp=inner_z)

    def a_copy(k):
        return remote(abuf.at[k], mb_in.at[k], a_s, a_r.at[k], tp=mid_z)

    def fz_copy(k):
        return remote(fall.at[sp, k], fall.at[sp, k], fz_s, fz_r.at[k], tp=end_z)

    def fy_copy(k, owner):
        return remote(fall.at[owner, k], fall.at[owner, k], fy_s, fy_r.at[k], sp=yn)

    def fs_copy(k, owner):
        return remote(fall.at[owner, k], fall.at[owner, k], fs_s, fs_r.at[k], sp=sib)

    def gs_copy(k, owner):
        return remote(fall.at[owner, k], fall.at[owner, k], gs_s, gs_r.at[k], sp=sib)

    def merge(r):
        d2d_copies[1][r].wait()
        y_copies[r].wait()
        base = pl.multiple_of(y * own_rows + r * rows, rows)
        for j in range(heads):
            near = combined(1, r, j) * fac_ref[1, pl.ds(base, rows), j:j + 1]
            far = y_in[r, :, j * 128:(j + 1) * 128] * fac_ref[1, pl.ds(base, rows), heads + j:heads + j + 1]
            obuf[r, :, j * 128:(j + 1) * 128] = (near + far).astype(jnp.bfloat16)

    def project(first):
        for k in range(first, first + GROUP):
            cols = slice(k % per_half * COLS, (k % per_half + 1) * COLS)
            pbuf[k] = jnp.dot(obuf[k // per_half], w_ref[:, cols], preferred_element_type=jnp.float32)

        @pl.when(is_end)
        def _():
            for k in range(first, first + GROUP):
                p_copy(k).start()

    def stage_a(k):
        @pl.when(inner)
        def _():
            p_copy(k).wait_recv()
            abuf[k] = pbuf[k] + pe_in[k]
            a_copy(k).start()

    def stage_f(k):
        @pl.when(inner)
        def _():
            a_copy(k).wait_recv()
            fall[sp, k] = abuf[k] + mb_in[k]
            fz_copy(k).start()

        @pl.when(is_end)
        def _():
            fz_copy(k).wait_recv()

        fy_copy(k, sp).start()
        fs_copy(k, sp).start()

    def stage_y(k):
        fy_copy(k, yn).wait_recv()
        gs_copy(k, yn).start()

    def stage_o(k):
        fs_copy(k, sib).wait_recv()
        gs_copy(k, diag).wait_recv()
        r, j = k // per_half, k % per_half
        cols = slice(j * COLS, (j + 1) * COLS)
        for owner in range(4):
            oy, oc = owner // 2, owner % 2
            start = oc * 2 * own_rows + oy * own_rows + r * rows
            out_ref[start:start + rows, cols] = (
                hid_ref[start:start + rows, cols].astype(jnp.float32) + fall[owner, k]).astype(jnp.bfloat16)

    w_copy.wait()
    for r in range(EARLY):
        merge(r)
        for first in range(r * per_half, (r + 1) * per_half, GROUP):
            project(first)
    hid_copy.wait()
    later = {}
    for r in range(EARLY, HALVES):
        later.setdefault(r - EARLY, []).append((merge, r))
        for i, first in enumerate(range(r * per_half, (r + 1) * per_half, GROUP)):
            later.setdefault(r - EARLY + i + (HALVES == 2), []).append((project, first))
    stages = tuple(zip((stage_a, stage_f, stage_y, stage_o), LAGS))
    for step in range(chunks + LAGS[-1]):
        for stage, lag in stages:
            if 0 <= step - lag < chunks:
                stage(step - lag)
        for task, which in later.get(step, ()):
            task(which)

    def all_sent(src, send, **where):
        remote(src, src, send, fs_r.at[0], **where).wait_send()

    @pl.when(inner)
    def _():
        all_sent(abuf, a_s, tp=mid_z)
        all_sent(fall.at[sp], fz_s, tp=end_z)

    @pl.when(is_end)
    def _():
        all_sent(pbuf, p_s, tp=inner_z)

    all_sent(fall.at[sp], fy_s, sp=yn)
    all_sent(fall.at[sp], fs_s, sp=sib)
    all_sent(fall.at[yn], gs_s, sp=sib)


def combine(acc, stats, hidden, w_out):
    batch, width = acc.shape
    features = w_out.shape[1]
    rows = batch // (4 * HALVES)
    chunks = HALVES * (features // COLS)
    dma = lambda *shape: pltpu.SemaphoreType.DMA(shape)
    f32 = lambda *shape: pltpu.VMEM(shape, jnp.float32)
    vmem, hbm = pl.BlockSpec(memory_space=pltpu.VMEM), pl.BlockSpec(memory_space=pltpu.HBM)
    return pl.pallas_call(
        combine_kernel,
        out_shape=jax.ShapeDtypeStruct((batch, features), jnp.bfloat16),
        in_specs=[vmem, vmem, hbm, hbm],
        out_specs=vmem,
        scratch_shapes=[
            pltpu.VMEM(hidden.shape, jnp.bfloat16),
            pltpu.VMEM(w_out.shape, jnp.bfloat16),
            f32(3, stats.shape[0], batch // 2),
            f32(2, batch // 2, batch // 2),
            f32(2, HALVES, rows, width),
            f32(HALVES, rows, width),
            f32(HALVES, rows, width),
            pltpu.VMEM((HALVES, rows, width), jnp.bfloat16),
            f32(chunks, rows, COLS),
            f32(chunks, rows, COLS),
            f32(chunks, rows, COLS),
            f32(chunks, rows, COLS),
            f32(4, chunks, rows, COLS),
            pltpu.SemaphoreType.DMA, pltpu.SemaphoreType.DMA, dma(3), dma(3), dma(2 * HALVES), dma(2 * HALVES), dma(HALVES), dma(HALVES),
        ] + [pltpu.SemaphoreType.DMA, dma(chunks)] * 6,
        compiler_params=pltpu.CompilerParams(collective_id=0, has_side_effects=True, vmem_limit_bytes=int(COMBINE_VMEM * 2**20)),
        name='combine',
    )(acc, stats, hidden, w_out)


def attend_kernel(len_hbm, hid_hbm, gain_hbm, wq_hbm, wk_hbm, wv_hbm, k_hbm, v_hbm, kout_hbm, vout_hbm, acc_ref, stats_ref,
                  hid, nbuf, wq, wk, wv, kbuf, vbuf, qbuf, nk, nv, statbuf, len_ref, gain_ref, hid_sem, wq_sem, wk_sem, wv_sem, k_sem, v_sem,
                  ko_sem, vo_sem, len_sem, gain_sem):
    batch, features = hid.shape
    heads = qbuf.shape[1] // 128
    base = lax.axis_index('sp') * BLOCK
    pieces = k_sem.shape[0]
    seqs = batch // pieces
    piece = seqs * BLOCK * 2
    copy = pltpu.make_async_copy
    quarter = batch // hid_sem.shape[0]
    hid_copies = [copy(hid_hbm.at[pl.ds(i * quarter, quarter), :], hid.at[pl.ds(i * quarter, quarter), :], hid_sem.at[i])
                  for i in range(hid_sem.shape[0])]
    wk_copy, wv_copy = copy(wk_hbm, wk, wk_sem), copy(wv_hbm, wv, wv_sem)
    wide, deep = 256, features // wq_sem.shape[0]
    wq_copies = [copy(wq_hbm.at[pl.ds(i * deep, deep), :], wq.at[pl.ds(i * deep, deep), :], wq_sem.at[i])
                 for i in range(wq_sem.shape[0])]

    def block_copy(src, dst, sem, i):
        rows = pl.ds(pl.multiple_of(i * piece, piece), piece)
        return copy(src.at[rows, :], dst.at[rows, :], sem.at[i])

    gain_copy, len_copy = copy(gain_hbm, gain_ref, gain_sem), copy(len_hbm, len_ref, len_sem)
    for c in [gain_copy, len_copy] + hid_copies + [wk_copy, wv_copy]:
        c.start()

    def norm_rows(i):
        rows = pl.ds(pl.multiple_of(i * 16, 16), 16)
        h = hid[rows, :].astype(jnp.float32)
        gain = gain_ref[...].astype(jnp.float32).reshape(1, features)
        inv_rms = lax.rsqrt(jnp.mean(h * h, axis=-1, keepdims=True) + EPS)
        nbuf[rows, :] = (h * inv_rms * gain).astype(jnp.bfloat16)

    for i, c in enumerate(hid_copies):
        c.wait()
        if i == 0:
            gain_copy.wait()
            len_copy.wait()
            for j in range(pieces):
                block_copy(k_hbm, kbuf, k_sem, j).start()
                block_copy(v_hbm, vbuf, v_sem, j).start()
        if i == 2:
            for w in wq_copies:
                w.start()
        per = quarter // 16
        pl.loop(i * per, (i + 1) * per)(norm_rows)

    for weight, weight_copy, out in ((wk, wk_copy, nk), (wv, wv_copy, nv)):
        weight_copy.wait()
        new = jnp.dot(nbuf[...], weight[...], preferred_element_type=jnp.float32)
        new = new.astype(jnp.bfloat16).astype(jnp.float32)
        for j in range(2):
            out[j] = new[:, j * 128:(j + 1) * 128]

    lane = lax.broadcasted_iota(jnp.int32, (8, 128), 1)
    row = lax.broadcasted_iota(jnp.int32, (8, 128), 0)
    slot_pos = base + (lane % 64) // 2
    own_seq = (lane // 64) == (row % 2)
    even = lane % 2 == 0
    pairs = [row // 2 == j for j in range(4)]
    odd_row = row % 2 == 1
    slot_row = lax.broadcasted_iota(jnp.int32, (16, 128), 0) // 2

    def place_new(g):
        group = pl.ds(pl.multiple_of(g * 8, 8), 8)
        news = [(new[0, group, :], new[1, group, :]) for new in (nk, nv)]
        spots = []
        for j in range(8):
            b = g * 8 + j
            at = len_ref[b] - base
            first = jnp.clip(at, 0, BLOCK - 1) // 8
            rows = pl.ds(pl.multiple_of(b * 2 * BLOCK + first * 16, 16), 16)
            spots.append((rows, slot_row == at - first * 8))
        olds = [(kbuf[rows, :], vbuf[rows, :]) for rows, _ in spots]
        for j, (rows, here) in enumerate(spots):
            for buf, (low, high), old in zip((kbuf, vbuf), news, olds[j]):
                fresh = jnp.where(odd_row, jnp.broadcast_to(high[j:j + 1], (8, 128)), jnp.broadcast_to(low[j:j + 1], (8, 128)))
                fresh = jnp.concatenate([fresh, fresh], axis=0)
                buf[rows, :] = jnp.where(here, fresh, old.astype(jnp.float32)).astype(jnp.bfloat16)

    def scores(i):
        seq8 = pl.ds(pl.multiple_of(i * 8, 8), 8)
        keys = pl.ds(pl.multiple_of(i * 512, 512), 512)
        q = jnp.concatenate([qbuf[seq8, h * 128:(h + 1) * 128] for h in range(heads)], axis=0).astype(jnp.bfloat16)
        s = lax.dot_general(q, kbuf[keys, :], (((1,), (1,)), ((), ())), preferred_element_type=jnp.float32)
        out = []
        for h in range(heads):
            part = [s[h * 8:(h + 1) * 8, j * 128:(j + 1) * 128] for j in range(4)]
            out.append(jnp.where(pairs[0], part[0], jnp.where(pairs[1], part[1], jnp.where(pairs[2], part[2], part[3]))))
        return out

    def softmax(i, score_list):
        seq8 = pl.ds(pl.multiple_of(i * 8, 8), 8)
        lens = jnp.full((8, 128), len_ref[i * 8], jnp.int32)
        for j in range(1, 8):
            lens = jnp.where(row == j, len_ref[i * 8 + j], lens)
        valid = jnp.logical_and(own_seq, slot_pos <= lens)
        valids = (jnp.logical_and(valid, even), jnp.logical_and(valid, jnp.logical_not(even)))
        oks = [valids[h // (heads // 2)] for h in range(heads)]
        masked = [jnp.where(ok, score * SCALE, NEG_BIG) for ok, score in zip(oks, score_list)]
        peaks = [jnp.max(score, axis=1, keepdims=True) for score in masked]
        exps = [jnp.where(ok, jnp.exp(score - peak), 0.0) for ok, score, peak in zip(oks, masked, peaks)]
        sums = [jnp.sum(e, axis=1, keepdims=True) for e in exps]
        stat = jnp.zeros((8, 128), jnp.float32)
        for h in range(heads):
            stat = jnp.where(lane == h, peaks[h], jnp.where(lane == heads + h, sums[h], stat))
        statbuf[seq8, :] = stat
        probs = [jnp.concatenate([jnp.where(pairs[j], e, 0.0) for j in range(4)], axis=1) for e in exps]
        return jnp.concatenate(probs, axis=0).astype(jnp.bfloat16)

    def values(i, p):
        seq8 = pl.ds(pl.multiple_of(i * 8, 8), 8)
        keys = pl.ds(pl.multiple_of(i * 512, 512), 512)
        o = jnp.dot(p, vbuf[keys, :], preferred_element_type=jnp.float32)
        for h in range(heads):
            acc_ref[seq8, h * 128:(h + 1) * 128] = o[h * 8:(h + 1) * 8, :]

    per_piece = seqs // 8

    @pl.loop(0, pieces)
    def _(i):
        block_copy(k_hbm, kbuf, k_sem, i).wait()
        block_copy(v_hbm, vbuf, v_sem, i).wait()

        @pl.loop(0, per_piece)
        def _(j):
            place_new(i * per_piece + j)

    for c in wq_copies:
        c.wait()
    for i in range(wq.shape[1] // wide):
        query = jnp.dot(nbuf[...], wq[:, i * wide:(i + 1) * wide], preferred_element_type=jnp.float32)
        qbuf[:, i * wide:(i + 1) * wide] = query.astype(jnp.bfloat16).astype(jnp.float32)

    for i in range(pieces):
        block_copy(kbuf, kout_hbm, ko_sem, i).start()
        block_copy(vbuf, vout_hbm, vo_sem, i).start()

    @pl.loop(0, pieces)
    def _(i):
        @pl.loop(0, per_piece, step=UNROLL)
        def _(j):
            tiles = [i * per_piece + j + u for u in range(UNROLL)]
            score_lists = [scores(t) for t in tiles]
            prob_list = [softmax(t, score_list) for t, score_list in zip(tiles, score_lists)]
            for t, p in zip(tiles, prob_list):
                values(t, p)

    for i in range(batch // 128):
        stats_ref[:, i * 128:(i + 1) * 128] = statbuf[i * 128:(i + 1) * 128, :].T[0:2 * heads, :]

    for i in range(pieces):
        block_copy(kbuf, kout_hbm, ko_sem, i).wait()
        block_copy(vbuf, vout_hbm, vo_sem, i).wait()


def attend(hidden, lengths, k_cache, v_cache, norm_gain, w_query, w_key, w_value):
    batch, block, kv, dim = k_cache.shape
    features, width = w_query.shape
    slots = batch * block * kv
    bf16 = lambda *shape: pltpu.VMEM(shape, jnp.bfloat16)
    f32 = lambda *shape: pltpu.VMEM(shape, jnp.float32)
    dma, one = lambda *shape: pltpu.SemaphoreType.DMA(shape), pltpu.SemaphoreType.DMA
    hbm, vmem = pl.BlockSpec(memory_space=pltpu.HBM), pl.BlockSpec(memory_space=pltpu.VMEM)
    cache = jax.ShapeDtypeStruct((slots, dim), jnp.bfloat16)
    k_new, v_new, acc, stats = pl.pallas_call(
        attend_kernel,
        out_shape=[cache, cache, jax.ShapeDtypeStruct((batch, width), jnp.float32),
                   jax.ShapeDtypeStruct((2 * width // dim, batch), jnp.float32)],
        in_specs=[hbm] * 8,
        out_specs=[hbm, hbm, vmem, vmem],
        scratch_shapes=[
            bf16(batch, features), bf16(batch, features), bf16(features, width), bf16(features, 256),
            bf16(features, 256), bf16(slots, dim), bf16(slots, dim), f32(batch, width), f32(kv, batch, dim),
            f32(kv, batch, dim), f32(batch, 128), pltpu.SMEM((batch,), jnp.int32), bf16(features),
            dma(4), dma(width // 256), one, one, dma(PIECES), dma(PIECES), dma(PIECES), dma(PIECES), one, one,
        ],
        compiler_params=pltpu.CompilerParams(vmem_limit_bytes=int(ATTEND_VMEM * 2**20)),
        name='attend',
    )(pltpu.with_memory_space_constraint(lengths, pltpu.HBM), hidden, pltpu.with_memory_space_constraint(norm_gain, pltpu.HBM), w_query, w_key, w_value, k_cache.reshape(slots, dim), v_cache.reshape(slots, dim))
    return k_new.reshape(k_cache.shape), v_new.reshape(v_cache.shape), acc, stats


def solution(mesh):
    cache_spec = P('dp', 'sp', 'tp', None)

    def local_step(hidden, lengths, k_cache, v_cache, norm_gain, w_query, w_key, w_value, w_out):
        k_new, v_new, acc, stats = attend(hidden, lengths, k_cache, v_cache, norm_gain, w_query, w_key, w_value)
        return combine(acc, stats, hidden, w_out), k_new, v_new

    return jax.shard_map(
        local_step,
        mesh=mesh,
        in_specs=(P('dp', None), P('dp'), cache_spec, cache_spec, P(None), P(None, 'tp'), P(None, 'tp'), P(None, 'tp'), P('tp', None)),
        out_specs=(P('dp', None), cache_spec, cache_spec),
        check_vma=False,
    )
```

```python
import jax
import jax.numpy as jnp
from jax import lax
from jax.experimental import pallas as pl
from jax.experimental.pallas import tpu as pltpu
from jax.sharding import PartitionSpec as P

EPS = 1e-6
NEG_BIG = -1e30
MESH = pl.DeviceIdType.MESH
HALVES = 4
EARLY = 1
COLS = 1024
GROUP = 4
BLOCK = 32
SCALE = 128 ** -0.5
UNROLL = 16
PIECES = 2
LAGS = (0, 3, 6, 8)
ATTEND_VMEM = 51.5
COMBINE_VMEM = 50


def combine_kernel(acc_ref, stats_ref, hid_hbm, w_hbm, out_ref, hid_ref, w_ref, stat_in, fac_ref, d2d_in, y_out, y_in, obuf, pbuf,
                   pe_in, abuf, mb_in, fall, h_sem, w_sem, st_s, st_r, dd_s, dd_r, yy_s, yy_r, p_s, p_r, a_s, a_r, fz_s, fz_r,
                   fy_s, fy_r, fs_s, fs_r, gs_s, gs_r):
    heads = acc_ref.shape[1] // 128
    rows = obuf.shape[1]
    own_rows = HALVES * rows
    per_half = out_ref.shape[1] // COLS
    chunks = HALVES * per_half
    sp = lax.axis_index('sp')
    z = lax.axis_index('tp')
    y, c = sp // 2, sp % 2
    sib, yn, diag = 2 * y + (1 - c), 2 * (1 - y) + c, 2 * (1 - y) + (1 - c)
    inner = jnp.logical_or(z == 1, z == 2)
    is_end = jnp.logical_or(z == 0, z == 3)
    low = z // 2
    end_z = low * 3
    mid_z = 2 - low
    inner_z = 1 + low

    hid_copy, w_copy = pltpu.make_async_copy(hid_hbm, hid_ref, h_sem), pltpu.make_async_copy(w_hbm, w_ref, w_sem)
    w_copy.start()
    hid_copy.start()

    barrier = pltpu.get_barrier_semaphore()
    for peer in (sib, yn, diag):
        pl.semaphore_signal(barrier, inc=1, device_id={'sp': peer}, device_id_type=MESH)

    @pl.when(inner)
    def _():
        pl.semaphore_signal(barrier, inc=1, device_id={'tp': end_z}, device_id_type=MESH)
        pl.semaphore_signal(barrier, inc=1, device_id={'tp': mid_z}, device_id_type=MESH)
        pl.semaphore_wait(barrier, 5)

    @pl.when(is_end)
    def _():
        pl.semaphore_signal(barrier, inc=1, device_id={'tp': inner_z}, device_id_type=MESH)
        pl.semaphore_wait(barrier, 4)

    def remote(src, dst, send, recv, **where):
        return pltpu.make_async_remote_copy(src_ref=src, dst_ref=dst, send_sem=send, recv_sem=recv, device_id=where,
                                            device_id_type=MESH)

    def stat_copy(i, peer):
        lanes = pl.ds(pl.multiple_of((peer % 2) * 2 * own_rows, 128), 2 * own_rows)
        return remote(stats_ref.at[:, lanes], stat_in.at[i], st_s, st_r.at[i], sp=peer)

    stat_copies = [stat_copy(i, peer) for i, peer in enumerate((sib, yn, diag))]
    for copy in stat_copies:
        copy.start()

    def d2d_copy(t, r):
        plane = (1 - y) if t == 0 else y
        start = pl.multiple_of((1 - c) * 2 * own_rows + plane * own_rows + r * rows, rows)
        return remote(acc_ref.at[pl.ds(start, rows), :], d2d_in.at[t, r], dd_s, dd_r.at[2 * r + t], sp=sib)

    d2d_copies = [[d2d_copy(t, r) for r in range(HALVES)] for t in range(2)]
    for t in range(2):
        for r in range(HALVES):
            d2d_copies[t][r].start()

    lanes = pl.ds(pl.multiple_of(c * 2 * own_rows, 128), 2 * own_rows)
    stat_copies[0].wait_recv()
    peaks = [stats_ref[0:heads, lanes], stat_in[0, 0:heads, :]]
    sums = [stats_ref[heads:2 * heads, lanes], stat_in[0, heads:2 * heads, :]]
    chip_top = jnp.maximum(peaks[0], peaks[1])
    unused = jnp.zeros((2 * own_rows - 2 * heads, 2 * own_rows), jnp.float32)
    fac_ref[0] = jnp.concatenate([jnp.exp(peaks[0] - chip_top), jnp.exp(peaks[1] - chip_top), unused], axis=0).T

    def combined(t, r, j):
        plane = (1 - y) if t == 0 else y
        base = pl.multiple_of(plane * own_rows + r * rows, rows)
        start = pl.multiple_of(c * 2 * own_rows + base, rows)
        cols = slice(j * 128, (j + 1) * 128)
        mine = acc_ref[pl.ds(start, rows), cols] * fac_ref[0, pl.ds(base, rows), j:j + 1]
        return mine + d2d_in[t, r, :, cols] * fac_ref[0, pl.ds(base, rows), heads + j:heads + j + 1]

    def y_copy(r):
        return remote(y_out.at[r], y_in.at[r], yy_s, yy_r.at[r], sp=yn)

    y_copies = [y_copy(r) for r in range(HALVES)]
    for r in range(HALVES):
        d2d_copies[0][r].wait_recv()
        for j in range(heads):
            y_out[r, :, j * 128:(j + 1) * 128] = combined(0, r, j)
        y_copies[r].start()

    for copy in stat_copies[1:]:
        copy.wait_recv()
    peaks += [stat_in[i, 0:heads, :] for i in (1, 2)]
    sums += [stat_in[i, heads:2 * heads, :] for i in (1, 2)]
    far_top = jnp.maximum(peaks[2], peaks[3])
    top = jnp.maximum(chip_top, far_top)
    parts = [one_sum * jnp.exp(peak - top) for one_sum, peak in zip(sums, peaks)]
    total = parts[0] + parts[1] + (parts[2] + parts[3])
    fac_ref[1] = jnp.concatenate([jnp.exp(chip_top - top) / total, jnp.exp(far_top - top) / total, unused], axis=0).T

    def p_copy(k):
        return remote(pbuf.at[k], pe_in.at[k], p_s, p_r.at[k], tp=inner_z)

    def a_copy(k):
        return remote(abuf.at[k], mb_in.at[k], a_s, a_r.at[k], tp=mid_z)

    def fz_copy(k):
        return remote(fall.at[sp, k], fall.at[sp, k], fz_s, fz_r.at[k], tp=end_z)

    def fy_copy(k, owner):
        return remote(fall.at[owner, k], fall.at[owner, k], fy_s, fy_r.at[k], sp=yn)

    def fs_copy(k, owner):
        return remote(fall.at[owner, k], fall.at[owner, k], fs_s, fs_r.at[k], sp=sib)

    def gs_copy(k, owner):
        return remote(fall.at[owner, k], fall.at[owner, k], gs_s, gs_r.at[k], sp=sib)

    def merge(r):
        d2d_copies[1][r].wait_recv()
        y_copies[r].wait_recv()
        base = pl.multiple_of(y * own_rows + r * rows, rows)
        for j in range(heads):
            near = combined(1, r, j) * fac_ref[1, pl.ds(base, rows), j:j + 1]
            far = y_in[r, :, j * 128:(j + 1) * 128] * fac_ref[1, pl.ds(base, rows), heads + j:heads + j + 1]
            obuf[r, :, j * 128:(j + 1) * 128] = (near + far).astype(jnp.bfloat16)

    def project(first):
        for k in range(first, first + GROUP):
            cols = slice(k % per_half * COLS, (k % per_half + 1) * COLS)
            pbuf[k] = jnp.dot(obuf[k // per_half], w_ref[:, cols], preferred_element_type=jnp.float32)

        @pl.when(is_end)
        def _():
            for k in range(first, first + GROUP):
                p_copy(k).start()

    def stage_a(k):
        @pl.when(inner)
        def _():
            p_copy(k).wait_recv()
            abuf[k] = pbuf[k] + pe_in[k]
            a_copy(k).start()

    def stage_f(k):
        @pl.when(inner)
        def _():
            a_copy(k).wait_recv()
            fall[sp, k] = abuf[k] + mb_in[k]
            fz_copy(k).start()

        @pl.when(is_end)
        def _():
            fz_copy(k).wait_recv()

        fy_copy(k, sp).start()
        fs_copy(k, sp).start()

    def stage_y(k):
        fy_copy(k, yn).wait_recv()
        gs_copy(k, yn).start()

    def stage_o(k):
        fs_copy(k, sib).wait_recv()
        gs_copy(k, diag).wait_recv()
        r, j = k // per_half, k % per_half
        cols = slice(j * COLS, (j + 1) * COLS)
        for owner in range(4):
            oy, oc = owner // 2, owner % 2
            start = oc * 2 * own_rows + oy * own_rows + r * rows
            out_ref[start:start + rows, cols] = (
                hid_ref[start:start + rows, cols].astype(jnp.float32) + fall[owner, k]).astype(jnp.bfloat16)

    w_copy.wait()
    for r in range(EARLY):
        merge(r)
        for first in range(r * per_half, (r + 1) * per_half, GROUP):
            project(first)
    hid_copy.wait()
    later = {}
    for r in range(EARLY, HALVES):
        later.setdefault(r - EARLY, []).append((merge, r))
        for i, first in enumerate(range(r * per_half, (r + 1) * per_half, GROUP)):
            later.setdefault(r - EARLY + i + (HALVES == 2), []).append((project, first))
    stages = tuple(zip((stage_a, stage_f, stage_y, stage_o), LAGS))
    for step in range(chunks + LAGS[-1]):
        for stage, lag in stages:
            if 0 <= step - lag < chunks:
                stage(step - lag)
        for task, which in later.get(step, ()):
            task(which)

    def all_sent(src, send, **where):
        remote(src, src, send, fs_r.at[0], **where).wait_send()

    @pl.when(inner)
    def _():
        all_sent(abuf, a_s, tp=mid_z)
        all_sent(fall.at[sp], fz_s, tp=end_z)

    @pl.when(is_end)
    def _():
        all_sent(pbuf, p_s, tp=inner_z)

    all_sent(stat_in, st_s, sp=sib)
    all_sent(d2d_in, dd_s, sp=sib)
    all_sent(y_out, yy_s, sp=yn)
    all_sent(fall.at[sp], fy_s, sp=yn)
    all_sent(fall.at[sp], fs_s, sp=sib)
    all_sent(fall.at[yn], gs_s, sp=sib)


def combine(acc, stats, hidden, w_out):
    batch, width = acc.shape
    features = w_out.shape[1]
    rows = batch // (4 * HALVES)
    chunks = HALVES * (features // COLS)
    dma = lambda *shape: pltpu.SemaphoreType.DMA(shape)
    f32 = lambda *shape: pltpu.VMEM(shape, jnp.float32)
    vmem, hbm = pl.BlockSpec(memory_space=pltpu.VMEM), pl.BlockSpec(memory_space=pltpu.HBM)
    return pl.pallas_call(
        combine_kernel,
        out_shape=jax.ShapeDtypeStruct((batch, features), jnp.bfloat16),
        in_specs=[vmem, vmem, hbm, hbm],
        out_specs=vmem,
        scratch_shapes=[
            pltpu.VMEM(hidden.shape, jnp.bfloat16),
            pltpu.VMEM(w_out.shape, jnp.bfloat16),
            f32(3, stats.shape[0], batch // 2),
            f32(2, batch // 2, batch // 2),
            f32(2, HALVES, rows, width),
            f32(HALVES, rows, width),
            f32(HALVES, rows, width),
            pltpu.VMEM((HALVES, rows, width), jnp.bfloat16),
            f32(chunks, rows, COLS),
            f32(chunks, rows, COLS),
            f32(chunks, rows, COLS),
            f32(chunks, rows, COLS),
            f32(4, chunks, rows, COLS),
            pltpu.SemaphoreType.DMA, pltpu.SemaphoreType.DMA, pltpu.SemaphoreType.DMA, dma(3), pltpu.SemaphoreType.DMA, dma(2 * HALVES), pltpu.SemaphoreType.DMA, dma(HALVES),
        ] + [pltpu.SemaphoreType.DMA, dma(chunks)] * 6,
        compiler_params=pltpu.CompilerParams(collective_id=0, has_side_effects=True, vmem_limit_bytes=int(COMBINE_VMEM * 2**20)),
        name='combine',
    )(acc, stats, hidden, w_out)


def attend_kernel(len_hbm, hid_hbm, gain_hbm, wq_hbm, wk_hbm, wv_hbm, k_hbm, v_hbm, kout_hbm, vout_hbm, acc_ref, stats_ref,
                  hid, nbuf, wq, wk, wv, kbuf, vbuf, qbuf, nk, nv, statbuf, len_ref, gain_ref, hid_sem, wq_sem, wk_sem, wv_sem, k_sem, v_sem,
                  ko_sem, vo_sem, len_sem, gain_sem):
    batch, features = hid.shape
    heads = qbuf.shape[1] // 128
    base = lax.axis_index('sp') * BLOCK
    pieces = k_sem.shape[0]
    seqs = batch // pieces
    piece = seqs * BLOCK * 2
    copy = pltpu.make_async_copy
    quarter = batch // hid_sem.shape[0]
    hid_copies = [copy(hid_hbm.at[pl.ds(i * quarter, quarter), :], hid.at[pl.ds(i * quarter, quarter), :], hid_sem.at[i])
                  for i in range(hid_sem.shape[0])]
    wk_copy, wv_copy = copy(wk_hbm, wk, wk_sem), copy(wv_hbm, wv, wv_sem)
    wide, deep = 256, features // wq_sem.shape[0]
    wq_copies = [copy(wq_hbm.at[pl.ds(i * deep, deep), :], wq.at[pl.ds(i * deep, deep), :], wq_sem.at[i])
                 for i in range(wq_sem.shape[0])]

    def block_copy(src, dst, sem, i):
        rows = pl.ds(pl.multiple_of(i * piece, piece), piece)
        return copy(src.at[rows, :], dst.at[rows, :], sem.at[i])

    gain_copy, len_copy = copy(gain_hbm, gain_ref, gain_sem), copy(len_hbm, len_ref, len_sem)
    for c in [gain_copy, len_copy] + hid_copies + [wk_copy, wv_copy]:
        c.start()

    def norm_rows(i):
        rows = pl.ds(pl.multiple_of(i * 16, 16), 16)
        h = hid[rows, :].astype(jnp.float32)
        gain = gain_ref[...].astype(jnp.float32).reshape(1, features)
        inv_rms = lax.rsqrt(jnp.mean(h * h, axis=-1, keepdims=True) + EPS)
        nbuf[rows, :] = (h * inv_rms * gain).astype(jnp.bfloat16)

    for i, c in enumerate(hid_copies):
        c.wait()
        if i == 0:
            gain_copy.wait()
            len_copy.wait()
            for j in range(pieces):
                block_copy(k_hbm, kbuf, k_sem, j).start()
                block_copy(v_hbm, vbuf, v_sem, j).start()
        if i == 2:
            for w in wq_copies:
                w.start()
        per = quarter // 16
        pl.loop(i * per, (i + 1) * per)(norm_rows)

    for weight, weight_copy, out in ((wk, wk_copy, nk), (wv, wv_copy, nv)):
        weight_copy.wait()
        new = jnp.dot(nbuf[...], weight[...], preferred_element_type=jnp.float32)
        new = new.astype(jnp.bfloat16).astype(jnp.float32)
        for j in range(2):
            out[j] = new[:, j * 128:(j + 1) * 128]

    lane = lax.broadcasted_iota(jnp.int32, (8, 128), 1)
    row = lax.broadcasted_iota(jnp.int32, (8, 128), 0)
    slot_pos = base + (lane % 64) // 2
    own_seq = (lane // 64) == (row % 2)
    even = lane % 2 == 0
    pairs = [row // 2 == j for j in range(4)]
    odd_row = row % 2 == 1
    slot_row = lax.broadcasted_iota(jnp.int32, (16, 128), 0) // 2

    def place_new(g):
        group = pl.ds(pl.multiple_of(g * 8, 8), 8)
        news = [(new[0, group, :], new[1, group, :]) for new in (nk, nv)]
        spots = []
        for j in range(8):
            b = g * 8 + j
            at = len_ref[b] - base
            first = jnp.clip(at, 0, BLOCK - 1) // 8
            rows = pl.ds(pl.multiple_of(b * 2 * BLOCK + first * 16, 16), 16)
            spots.append((rows, slot_row == at - first * 8))
        olds = [(kbuf[rows, :], vbuf[rows, :]) for rows, _ in spots]
        for j, (rows, here) in enumerate(spots):
            for buf, (low, high), old in zip((kbuf, vbuf), news, olds[j]):
                fresh = jnp.where(odd_row, jnp.broadcast_to(high[j:j + 1], (8, 128)), jnp.broadcast_to(low[j:j + 1], (8, 128)))
                fresh = jnp.concatenate([fresh, fresh], axis=0)
                buf[rows, :] = jnp.where(here, fresh, old.astype(jnp.float32)).astype(jnp.bfloat16)

    def scores(i):
        seq8 = pl.ds(pl.multiple_of(i * 8, 8), 8)
        keys = pl.ds(pl.multiple_of(i * 512, 512), 512)
        q = jnp.concatenate([qbuf[seq8, h * 128:(h + 1) * 128] for h in range(heads)], axis=0).astype(jnp.bfloat16)
        s = lax.dot_general(q, kbuf[keys, :], (((1,), (1,)), ((), ())), preferred_element_type=jnp.float32)
        out = []
        for h in range(heads):
            part = [s[h * 8:(h + 1) * 8, j * 128:(j + 1) * 128] for j in range(4)]
            out.append(jnp.where(pairs[0], part[0], jnp.where(pairs[1], part[1], jnp.where(pairs[2], part[2], part[3]))))
        return out

    def softmax(i, score_list):
        seq8 = pl.ds(pl.multiple_of(i * 8, 8), 8)
        lens = jnp.full((8, 128), len_ref[i * 8], jnp.int32)
        for j in range(1, 8):
            lens = jnp.where(row == j, len_ref[i * 8 + j], lens)
        valid = jnp.logical_and(own_seq, slot_pos <= lens)
        valids = (jnp.logical_and(valid, even), jnp.logical_and(valid, jnp.logical_not(even)))
        oks = [valids[h // (heads // 2)] for h in range(heads)]
        masked = [jnp.where(ok, score * SCALE, NEG_BIG) for ok, score in zip(oks, score_list)]
        peaks = [jnp.max(score, axis=1, keepdims=True) for score in masked]
        exps = [jnp.where(ok, jnp.exp(score - peak), 0.0) for ok, score, peak in zip(oks, masked, peaks)]
        sums = [jnp.sum(e, axis=1, keepdims=True) for e in exps]
        stat = jnp.zeros((8, 128), jnp.float32)
        for h in range(heads):
            stat = jnp.where(lane == h, peaks[h], jnp.where(lane == heads + h, sums[h], stat))
        statbuf[seq8, :] = stat
        probs = [jnp.concatenate([jnp.where(pairs[j], e, 0.0) for j in range(4)], axis=1) for e in exps]
        return jnp.concatenate(probs, axis=0).astype(jnp.bfloat16)

    def values(i, p):
        seq8 = pl.ds(pl.multiple_of(i * 8, 8), 8)
        keys = pl.ds(pl.multiple_of(i * 512, 512), 512)
        o = jnp.dot(p, vbuf[keys, :], preferred_element_type=jnp.float32)
        for h in range(heads):
            acc_ref[seq8, h * 128:(h + 1) * 128] = o[h * 8:(h + 1) * 8, :]

    per_piece = seqs // 8

    @pl.loop(0, pieces)
    def _(i):
        block_copy(k_hbm, kbuf, k_sem, i).wait()
        block_copy(v_hbm, vbuf, v_sem, i).wait()

        @pl.loop(0, per_piece)
        def _(j):
            place_new(i * per_piece + j)

    for c in wq_copies:
        c.wait()
    for i in range(wq.shape[1] // wide):
        query = jnp.dot(nbuf[...], wq[:, i * wide:(i + 1) * wide], preferred_element_type=jnp.float32)
        qbuf[:, i * wide:(i + 1) * wide] = query.astype(jnp.bfloat16).astype(jnp.float32)

    for i in range(pieces):
        block_copy(kbuf, kout_hbm, ko_sem, i).start()
        block_copy(vbuf, vout_hbm, vo_sem, i).start()

    @pl.loop(0, pieces)
    def _(i):
        @pl.loop(0, per_piece, step=UNROLL)
        def _(j):
            tiles = [i * per_piece + j + u for u in range(UNROLL)]
            score_lists = [scores(t) for t in tiles]
            prob_list = [softmax(t, score_list) for t, score_list in zip(tiles, score_lists)]
            for t, p in zip(tiles, prob_list):
                values(t, p)

    for i in range(batch // 128):
        stats_ref[:, i * 128:(i + 1) * 128] = statbuf[i * 128:(i + 1) * 128, :].T[0:2 * heads, :]

    for i in range(pieces):
        block_copy(kbuf, kout_hbm, ko_sem, i).wait()
        block_copy(vbuf, vout_hbm, vo_sem, i).wait()


def attend(hidden, lengths, k_cache, v_cache, norm_gain, w_query, w_key, w_value):
    batch, block, kv, dim = k_cache.shape
    features, width = w_query.shape
    slots = batch * block * kv
    bf16 = lambda *shape: pltpu.VMEM(shape, jnp.bfloat16)
    f32 = lambda *shape: pltpu.VMEM(shape, jnp.float32)
    dma, one = lambda *shape: pltpu.SemaphoreType.DMA(shape), pltpu.SemaphoreType.DMA
    hbm, vmem = pl.BlockSpec(memory_space=pltpu.HBM), pl.BlockSpec(memory_space=pltpu.VMEM)
    cache = jax.ShapeDtypeStruct((slots, dim), jnp.bfloat16)
    k_new, v_new, acc, stats = pl.pallas_call(
        attend_kernel,
        out_shape=[cache, cache, jax.ShapeDtypeStruct((batch, width), jnp.float32),
                   jax.ShapeDtypeStruct((2 * width // dim, batch), jnp.float32)],
        in_specs=[hbm] * 8,
        out_specs=[hbm, hbm, vmem, vmem],
        scratch_shapes=[
            bf16(batch, features), bf16(batch, features), bf16(features, width), bf16(features, 256),
            bf16(features, 256), bf16(slots, dim), bf16(slots, dim), f32(batch, width), f32(kv, batch, dim),
            f32(kv, batch, dim), f32(batch, 128), pltpu.SMEM((batch,), jnp.int32), bf16(features),
            dma(4), dma(width // 256), one, one, dma(PIECES), dma(PIECES), dma(PIECES), dma(PIECES), one, one,
        ],
        compiler_params=pltpu.CompilerParams(vmem_limit_bytes=int(ATTEND_VMEM * 2**20)),
        name='attend',
    )(pltpu.with_memory_space_constraint(lengths, pltpu.HBM), hidden, pltpu.with_memory_space_constraint(norm_gain, pltpu.HBM), w_query, w_key, w_value, k_cache.reshape(slots, dim), v_cache.reshape(slots, dim))
    return k_new.reshape(k_cache.shape), v_new.reshape(v_cache.shape), acc, stats


def solution(mesh):
    cache_spec = P('dp', 'sp', 'tp', None)

    def local_step(hidden, lengths, k_cache, v_cache, norm_gain, w_query, w_key, w_value, w_out):
        k_new, v_new, acc, stats = attend(hidden, lengths, k_cache, v_cache, norm_gain, w_query, w_key, w_value)
        return combine(acc, stats, hidden, w_out), k_new, v_new

    return jax.shard_map(
        local_step,
        mesh=mesh,
        in_specs=(P('dp', None), P('dp'), cache_spec, cache_spec, P(None), P(None, 'tp'), P(None, 'tp'), P(None, 'tp'), P('tp', None)),
        out_specs=(P('dp', None), cache_spec, cache_spec),
        check_vma=False,
    )
```
